256 devices in a mesh: dp: 32 (over z_hi, x, core), tensor: 8 (over z_lo, y).
Axes of the slice: x: 4, y: 4, z: 8 (z_hi: 4, z_lo: 2; z = z_hi * 2 + z_lo), core: 2. Of those that a mesh axis runs over, the one named last changes fastest.
Arguments:
- query_rows: bfloat16 [12288, 5120], P('dp', 'tensor'), may hold values from -128 to 128
- key_rows: bfloat16 [12288, 5120], P('dp', 'tensor'), may hold values from -5 to 5
- value_rows: bfloat16 [12288, 5120], P('dp', 'tensor'), may hold values from -12 to 12
- action_mask: int32 [32, 384], P('dp'), may hold values from 0 to 1, as said below
- residual: bfloat16 [12288, 5120], P('dp', 'tensor'), may hold values from -100 to 100
- out_weight: bfloat16 [5120, 5120], P(None, 'tensor'), may hold values from -0.078125 to 0.078125
- norm_gain: float32 [5120], P('tensor'), may hold values from 0.1 to 1.9
- upstream: bfloat16 [12288, 5120], P('dp', 'tensor'), may hold values from -6 to 6
- residual_grad: bfloat16 [12288, 5120], P('dp', 'tensor'), may hold values from -2 to 2
Outputs:
- layer_out: bfloat16 [12288, 5120], P('dp', 'tensor')
- grad_residual: bfloat16 [12288, 5120], P('dp', 'tensor')
- grad_query: bfloat16 [12288, 5120], P('dp', 'tensor')
- grad_key: bfloat16 [12288, 5120], P('dp', 'tensor')
- grad_value: bfloat16 [12288, 5120], P('dp', 'tensor')
- grad_out_weight: float32 [5120, 5120], P('dp', 'tensor')
- grad_gain: float32 [5120], P('tensor')
The draws below stay inside these ranges and needn't reach their ends.
Inputs may be any that keep to these rules, and one draw needn't show every extreme that they name: `action_mask`: each row is a run of zeros followed by a run of ones; the ones number 1 to 192.
All inputs are finite; a program needn't handle non-finite values.
Results may differ from the reference program's by a relative error of at most 0.015.
Values may be sent and summed in bfloat16 or wider, within the bound.
A program may use at most 128 MiB of HBM per device.

```python
import jax
import jax.numpy as jnp
from jax import lax

D = 5120
HEADS = 40
HEAD_DIM = 128
LEN = 384
SEQS = 32
TOKENS = 12288


def attention_inputs(key):
    base_key = jax.random.fold_in(key, 17)
    key_query, key_key = jax.random.split(base_key, 2)
    shape = (SEQS, LEN, HEADS, HEAD_DIM)
    query_draw = jax.random.truncated_normal(key_query, -4.0, 4.0, shape, jnp.float32)
    key_draw = jax.random.truncated_normal(key_key, -4.0, 4.0, shape, jnp.float32)
    width = HEADS * HEAD_DIM
    return (query_draw.reshape(TOKENS, width), key_draw.reshape(TOKENS, width))


def draw_query_rows(key, part):
    return attention_inputs(key)[0].astype(jnp.bfloat16)


def draw_key_rows(key, part):
    return attention_inputs(key)[1].astype(jnp.bfloat16)


def draw_residual(key, part):
    key_base, key_rows = jax.random.split(jax.random.fold_in(key, 29), 2)
    columns = jnp.arange(D).astype(jnp.float32)
    column_scale = 10.0 ** (0.5 * columns / (D - 1))
    row_scale = jnp.exp(jax.random.uniform(key_rows, (TOKENS, 1), jnp.float32, jnp.log(0.5), jnp.log(5.0)))
    base = jax.random.truncated_normal(key_base, -5.0, 5.0, (TOKENS, D), jnp.float32)
    return (base * row_scale * column_scale[None, :]).astype(jnp.bfloat16)


def draw_action_mask(key, part):
    actions = jax.random.randint(jax.random.fold_in(key, 41), (SEQS,), 1, LEN // 2 + 1)
    position = jnp.arange(LEN)
    return (position[None, :] >= LEN - actions[:, None]).astype(jnp.int32)


def spiked(drawn, stream_key, source, target, parts, factor):
    def block_of(dim):
        return (jnp.arange(drawn.shape[dim]) // (drawn.shape[dim] // parts)).reshape((-1,) + (1,) * (drawn.ndim - 1 - dim))

    first = jax.random.permutation(stream_key, parts)[block_of(target)]
    far = (block_of(target) + parts // 2) % parts
    return jnp.where((block_of(source) == first) | (block_of(source) == far), factor * drawn, drawn)


def steps_of(rng, extent, shards, least, high):
    def one(dim, parts):
        heights = jax.random.uniform(jax.random.fold_in(jax.random.fold_in(rng, 6), dim), (parts,), jnp.float32, least / len(shards), high / len(shards))
        return jnp.repeat(jnp.exp(heights), extent[dim] // parts).reshape((-1,) + (1,) * (len(extent) - dim - 1))

    factor_of = one(*shards[0])
    for cut in shards[1:]:
        factor_of = factor_of * one(*cut)
    return factor_of


def centred(own_key, extent, scale, reach, cuts=(), held_as=jnp.bfloat16):
    result = scale * jax.random.normal(own_key, extent, jnp.float32)
    if cuts:
        result = result * steps_of(own_key, extent, cuts, -0.22, 0.18)
    return jnp.clip(result, -reach, reach).astype(held_as)


def gaussian_with(key, shape, scale, most, shards, heavy, kind=jnp.bfloat16):
    drawn = scale * jax.random.normal(key, shape, jnp.float32)
    if shards:
        drawn = drawn * steps_of(key, shape, shards, -0.22, 0.18)
    return jnp.clip(spiked(drawn, jax.random.fold_in(key, 3), *heavy), -most, most).astype(kind)


def setup_inputs(seed: int = 0) -> dict:
    key_of = jax.random.split(jax.random.key(seed), 10)
    return {
        "query_rows": draw_query_rows(jax.random.fold_in(key_of[9], 71), 0),
        "key_rows": draw_key_rows(jax.random.fold_in(key_of[9], 71), 0),
        "value_rows": centred(key_of[2], (TOKENS, HEADS * HEAD_DIM), 2.0, 12.0, ((0, 32), (1, 8))),
        "action_mask": draw_action_mask(jax.random.fold_in(key_of[9], 71), 0),
        "residual": draw_residual(jax.random.fold_in(key_of[9], 71), 0),
        "out_weight": centred(key_of[5], (D, HEADS * HEAD_DIM), (HEADS * HEAD_DIM) ** -0.5, 0.078125, ((1, 8),)),
        "norm_gain": jnp.clip(1.0 + 0.18 * jax.random.normal(key_of[6], (D,), jnp.float32), 0.1, 1.9),
        "upstream": gaussian_with(key_of[7], (TOKENS, D), 1.0, 6.0, ((0, 32), (1, 8)), (0, 1, 32, 2.75)),
        "residual_grad": centred(key_of[8], (TOKENS, D), 0.3, 2.0, ((0, 32), (1, 8))),
    }


epsilon = 1e-05

def visible(mask_row):
    position = jnp.arange(mask_row.shape[0])
    causal = position[None, :] <= position[:, None]
    observe = mask_row == 0
    return causal | observe[:, None] & observe[None, :]

def softmax_rows(query_heads, keyset, allowed):
    scores = jnp.einsum('qhd,khd->hqk', query_heads.astype(jnp.float32), keyset.astype(jnp.float32)) * HEAD_DIM ** (-0.5)
    masked = jnp.where(allowed[None], scores, -jnp.inf)
    row_top = lax.optimization_barrier(jnp.max(masked, axis=-1, keepdims=True))
    weights = jnp.exp(masked - row_top)
    return weights / lax.optimization_barrier(jnp.sum(weights, axis=-1, keepdims=True))

def split_heads(rows):
    return rows.reshape(LEN, HEADS, HEAD_DIM)

def forward_seq(inputs):
    query_seq, key_seq, value_seq, mask_row = inputs
    chances = softmax_rows(split_heads(query_seq), split_heads(key_seq), visible(mask_row))
    chances_low = lax.optimization_barrier(chances.astype(jnp.bfloat16)).astype(jnp.float32)
    attended = jnp.einsum('hqk,khd->qhd', chances_low, split_heads(value_seq).astype(jnp.float32))
    return attended.astype(jnp.bfloat16).reshape(LEN, HEADS * HEAD_DIM)

def backward_seq(inputs):
    query_seq, key_seq, value_seq, mask_row, grad_seq = inputs
    query_heads = split_heads(query_seq)
    key_heads = split_heads(key_seq)
    chances = softmax_rows(query_heads, key_heads, visible(mask_row))
    chances_low = lax.optimization_barrier(chances.astype(jnp.bfloat16)).astype(jnp.float32)
    grad_heads = split_heads(grad_seq).astype(jnp.float32)
    grad_value = jnp.einsum('hqk,qhd->khd', chances_low, grad_heads).astype(jnp.bfloat16)
    grad_chances = jnp.einsum('qhd,khd->hqk', grad_heads, split_heads(value_seq).astype(jnp.float32))
    row_delta = lax.optimization_barrier(jnp.sum(chances * grad_chances, axis=-1, keepdims=True))
    grad_scores = (chances * (grad_chances - row_delta) * HEAD_DIM ** (-0.5)).astype(jnp.bfloat16)
    grad_scores = lax.optimization_barrier(grad_scores).astype(jnp.float32)
    grad_query = jnp.einsum('hqk,khd->qhd', grad_scores, key_heads.astype(jnp.float32)).astype(jnp.bfloat16)
    grad_key = jnp.einsum('hqk,qhd->khd', grad_scores, query_heads.astype(jnp.float32)).astype(jnp.bfloat16)
    width = HEADS * HEAD_DIM
    return (grad_query.reshape(LEN, width), grad_key.reshape(LEN, width), grad_value.reshape(LEN, width))

def reference(query_rows, key_rows, value_rows, action_mask, residual, out_weight, norm_gain, upstream, residual_grad):
    width = HEADS * HEAD_DIM
    query_seq = query_rows.reshape(SEQS, LEN, width)
    key_seq = key_rows.reshape(SEQS, LEN, width)
    value_seq = value_rows.reshape(SEQS, LEN, width)
    attended = lax.map(forward_seq, (query_seq, key_seq, value_seq, action_mask)).reshape(TOKENS, width)
    projected = jnp.dot(attended, out_weight.T, preferred_element_type=jnp.float32)
    layer_out = (projected + residual.astype(jnp.float32)).astype(jnp.bfloat16)
    out_float = layer_out.astype(jnp.float32)
    row_rms = jnp.sqrt(lax.optimization_barrier(jnp.mean(out_float * out_float, axis=1, keepdims=True)) + epsilon)
    normed = out_float / row_rms
    scaled = upstream.astype(jnp.float32) * norm_gain[None, :]
    row_inner = lax.optimization_barrier(jnp.sum(scaled * out_float, axis=1, keepdims=True)) / (row_rms * D)
    grad_residual = (residual_grad.astype(jnp.float32) + (scaled - normed * row_inner) / row_rms).astype(jnp.bfloat16)
    grad_gain = lax.optimization_barrier(jnp.sum(upstream.astype(jnp.float32) * normed, axis=0))
    grad_out_weight = lax.dot_general(grad_residual, attended, (((0,), (0,)), ((), ())), preferred_element_type=jnp.float32)
    grad_attended = jnp.dot(grad_residual, out_weight, preferred_element_type=jnp.float32).astype(jnp.bfloat16)
    grad_seq = grad_attended.reshape(SEQS, LEN, width)
    grad_query, grad_key, grad_value = lax.map(backward_seq, (query_seq, key_seq, value_seq, action_mask, grad_seq))
    return (layer_out, grad_residual, grad_query.reshape(TOKENS, width), grad_key.reshape(TOKENS, width), grad_value.reshape(TOKENS, width), grad_out_weight, grad_gain)
```

```python
import functools

import jax
import jax.numpy as jnp
from jax import lax
from jax.experimental import pallas as pl
from jax.experimental.pallas import tpu as pltpu
from jax.sharding import PartitionSpec as P

MESH = pl.DeviceIdType.MESH
F32 = jnp.float32
BF16 = jnp.bfloat16

D = 5120
HEAD_DIM = 128
LEN = 384
WIDTH = 640
HEADS = WIDTH // HEAD_DIM
CA = 256
CB = WIDTH - CA
HALF = LEN // 2
OUT_ROWS = 160
HALF_ROWS = OUT_ROWS // 2
SCALE = HEAD_DIM ** (-0.5)
EPSILON = 1e-05
MESSAGES = 128


def dot(a, b, ca, cb):
    return lax.dot_general(a, b, (((ca,), (cb,)), ((), ())), preferred_element_type=F32)


def kernel(
    q_hbm, k_hbm, v_hbm, mask_ref, res_hbm, w_hbm, gain_ref, ups_hbm, rg_hbm,
    lo_hbm, gr_hbm, gq_hbm, gk_hbm, gv_hbm, gw_hbm, gg_ref,
    q, k, v, res, w, ups, rg, bias, probs, att, lo, gr, ga, gacc, gq, gk, gv, gw_out,
    pa, pb, rec_az, rec_a, rec_b, mer_a, mer_b, zb_send, zb_rec, own,
    stat, stat_rec, all_a, all_b,
    gwb, cx_rec, u, x_rec, x_mer, z_send, z_rec, z_own,
    gain0, gain0_rec, gain1, gain1_rec, gain2, gain2_rec,
    ssem, rsem, lsem,
):
    t = lax.axis_index("tensor")
    dp = lax.axis_index("dp")
    z, y = t // 4, t % 4
    c, x, zh = dp % 2, (dp // 2) % 4, dp // 8

    def at_y(step):
        return {"tensor": z * 4 + (y + step) % 4}

    z_peer = {"tensor": (1 - z) * 4 + y}
    c_peer = {"dp": dp + 1 - 2 * c}

    def at_x(step):
        return {"dp": zh * 8 + ((x + step) % 4) * 2 + c}

    def at_zh(step):
        return {"dp": ((zh + step) % 4) * 8 + x * 2 + c}

    peers = [{"tensor": (t + j) % 8} for j in range(1, 8)]
    peers += [c_peer]
    peers += [at_x(s) for s in (1, 2, 3)]
    peers += [at_zh(s) for s in (1, 2, 3)]

    local = []

    def fetch(src, dst):
        copy = pltpu.make_async_copy(src, dst, lsem.at[len(local)])
        local.append(copy)
        copy.start()
        return copy

    in_q, in_k, in_v = fetch(q_hbm, q), fetch(k_hbm, k), fetch(v_hbm, v)
    in_w = fetch(w_hbm, w)
    in_res, in_ups, in_rg = fetch(res_hbm, res), fetch(ups_hbm, ups), fetch(rg_hbm, rg)

    barrier = pltpu.get_barrier_semaphore()
    for peer in peers:
        pl.semaphore_signal(barrier, inc=1, device_id=peer, device_id_type=MESH)

    messages = []

    def message(src, dst, device, start=True):
        i = len(messages)
        copy = pltpu.make_async_remote_copy(
            src_ref=src, dst_ref=dst, send_sem=ssem.at[i], recv_sem=rsem.at[i],
            device_id=device, device_id_type=MESH,
        )
        messages.append(copy)
        if start:
            copy.start()
        return copy

    zeros = jnp.sum(1 - mask_ref[...], axis=1, keepdims=True)
    row = lax.broadcasted_iota(jnp.int32, (LEN, LEN), 0)
    col = lax.broadcasted_iota(jnp.int32, (LEN, LEN), 1)
    allowed = (col <= row) | (jnp.maximum(row, col) < zeros)
    bias[...] = jnp.where(allowed, 0.0, -jnp.inf).astype(F32)
    in_q.wait()
    in_k.wait()
    in_v.wait()

    def head_cols(h):
        return pl.ds(pl.multiple_of(h * HEAD_DIM, HEAD_DIM), HEAD_DIM)

    def forward(h, carry):
        cols = head_cols(h)
        s = dot(q[:, cols], k[:, cols], 1, 1) * SCALE + bias[...]
        e = jnp.exp(s - jnp.max(s, axis=1, keepdims=True))
        p = e * (1.0 / jnp.sum(e, axis=1, keepdims=True))
        probs[h] = p
        att[:, cols] = dot(p.astype(BF16), v[:, cols], 1, 0).astype(BF16)
        return carry

    lax.fori_loop(0, HEADS, forward, 0)
    in_w.wait()

    def w_rows(block):
        return pl.ds(pl.multiple_of(block * WIDTH, WIDTH), WIDTH)

    def project(d):
        def one(j, carry):
            zz = j * z + (1 - j) * (1 - z)
            block = zz * 4 + (y + d) % 4
            r = dot(att[...], w[w_rows(block), :], 1, 1)
            pa[d, j] = r[:, :CA].astype(BF16)
            pb[d, zz] = r[:, CA:].astype(BF16)
            return carry

        lax.fori_loop(0, 2, one, 0)

    first, second = pl.ds(0, HALF), pl.ds(HALF, HALF)
    az, b1, b2, a1, a2 = {}, {}, {}, {}, {}
    project(2)
    pl.semaphore_wait(barrier, len(peers))
    b1[1] = message(pb.at[2, :, first], rec_b.at[0], at_y(1))
    b1[-1] = message(pb.at[2, :, second], rec_b.at[1], at_y(-1))
    az[2] = message(pa.at[2, 0], rec_az.at[2], z_peer)
    project(1)
    b2[1] = message(pb.at[1, :, second], rec_b.at[2], at_y(1))
    az[1] = message(pa.at[1, 0], rec_az.at[1], z_peer)
    project(3)
    b2[-1] = message(pb.at[3, :, first], rec_b.at[3], at_y(-1))
    az[3] = message(pa.at[3, 0], rec_az.at[3], z_peer)
    project(0)
    az[0] = message(pa.at[0, 0], rec_az.at[0], z_peer)

    b1[1].wait_recv()
    mer_b[0] = pb[1, :, :HALF] + rec_b[0]
    b3 = {1: message(mer_b.at[0], rec_b.at[4], at_y(1))}
    b1[-1].wait_recv()
    mer_b[1] = pb[3, :, HALF:] + rec_b[1]
    b3[-1] = message(mer_b.at[1], rec_b.at[5], at_y(-1))

    def join(d):
        az[d].wait_recv()
        pa[d, 1] = pa[d, 1] + rec_az[d]

    join(2)
    a1[1] = message(pa.at[2, 1, first], rec_a.at[0], at_y(1))
    a1[-1] = message(pa.at[2, 1, second], rec_a.at[1], at_y(-1))
    join(1)
    a2[1] = message(pa.at[1, 1, second], rec_a.at[2], at_y(1))
    join(3)
    a2[-1] = message(pa.at[3, 1, first], rec_a.at[3], at_y(-1))
    az[0].wait_recv()

    b2[1].wait_recv()
    b2[-1].wait_recv()
    b3[1].wait_recv()
    b3[-1].wait_recv()

    def b_sum(zz):
        top = pb[0, zz, :HALF].astype(F32) + rec_b[3, zz].astype(F32) + rec_b[4, zz].astype(F32)
        low = pb[0, zz, HALF:].astype(F32) + rec_b[2, zz].astype(F32) + rec_b[5, zz].astype(F32)
        return top, low

    top, low = b_sum(1 - z)
    zb_send[:HALF] = top.astype(BF16)
    zb_send[HALF:] = low.astype(BF16)
    zb = message(zb_send, zb_rec, z_peer)

    a1[1].wait_recv()
    mer_a[0] = pa[1, 1, :HALF] + rec_a[0]
    a3 = {1: message(mer_a.at[0], rec_a.at[4], at_y(1))}
    a1[-1].wait_recv()
    mer_a[1] = pa[3, 1, HALF:] + rec_a[1]
    a3[-1] = message(mer_a.at[1], rec_a.at[5], at_y(-1))

    in_res.wait()
    in_ups.wait()
    in_rg.wait()
    top, low = b_sum(z)
    own[:HALF, CA:] = top
    own[HALF:, CA:] = low
    own[:, :CA] = pa[0, 1].astype(F32) + rec_az[0].astype(F32)

    zb.wait_recv()
    own_b = own[:, CA:] + zb_rec[...].astype(F32) + res[:, CA:].astype(F32)
    low_b = own_b.astype(BF16)
    lo[:, CA:] = low_b
    f_b = low_b.astype(F32)
    scaled_b = ups[:, CA:].astype(F32) * gain_ref[:, CA:]
    square = jnp.sum(f_b * f_b, axis=1, keepdims=True)
    inner = jnp.sum(f_b * scaled_b, axis=1, keepdims=True)

    a2[1].wait_recv()
    a2[-1].wait_recv()
    a3[1].wait_recv()
    a3[-1].wait_recv()
    top = own[:HALF, :CA] + rec_a[3].astype(F32) + rec_a[4].astype(F32) + res[:HALF, :CA].astype(F32)
    low = own[HALF:, :CA] + rec_a[2].astype(F32) + rec_a[5].astype(F32) + res[HALF:, :CA].astype(F32)
    lo[:HALF, :CA] = top.astype(BF16)
    lo[HALF:, :CA] = low.astype(BF16)
    f_a = lo[:, :CA].astype(F32)
    scaled_a = ups[:, :CA].astype(F32) * gain_ref[:, :CA]
    square = square + jnp.sum(f_a * f_a, axis=1, keepdims=True)
    inner = inner + jnp.sum(f_a * scaled_a, axis=1, keepdims=True)

    lane = lax.broadcasted_iota(jnp.int32, (LEN, 128), 1)
    packed = jnp.where(lane == 0, square, jnp.where(lane == 1, inner, 0.0))
    stat[...] = packed.T[:8]
    stats = [message(stat, stat_rec.at[j], peers[j - 1]) for j in range(1, 8)]
    out_lo = fetch(lo, lo_hbm)
    total = stat[...]
    for j in range(1, 8):
        stats[j - 1].wait_recv()
        total = total + stat_rec[j]
    wide = jnp.concatenate([total, jnp.zeros((120, LEN), F32)], axis=0).T
    square, inner = wide[:, 0:1], wide[:, 1:2]
    rms = jnp.sqrt(square / D + EPSILON)
    back = 1.0 / rms
    row_inner = inner / (rms * D)

    def grad_rows(lo_part, ups_part, gain_part, rg_part):
        up = ups_part.astype(F32)
        normed = lo_part.astype(F32) * back
        g = rg_part.astype(F32) + (up * gain_part - normed * row_inner) * back
        return g.astype(BF16), (up * normed).reshape(LEN // 8, 8, -1).sum(axis=0)

    g, gain_a = grad_rows(lo[:, :CA], ups[:, :CA], gain_ref[:, :CA], rg[:, :CA])
    all_a[t] = g
    gr[:, :CA] = g
    mine_a = all_a.at[t]
    first_a = all_a.at[t, first]
    second_a = all_a.at[t, second]
    y1 = {}
    y1["a", 1, 1] = message(first_a, first_a, at_y(1))
    y1["a", -1, 1] = message(second_a, second_a, at_y(-1))
    g, gain_b = grad_rows(lo[:, CA:], ups[:, CA:], gain_ref[:, CA:], rg[:, CA:])
    all_b[t] = g
    gr[:, CA:] = g
    zx_b = message(all_b.at[t], all_b.at[t], z_peer)
    zx_a = {0: message(mine_a, mine_a, z_peer)}
    first_b = all_b.at[t, first]
    second_b = all_b.at[t, second]
    y1["b", 1, 1] = message(first_b, first_b, at_y(1))
    y1["b", -1, 1] = message(second_b, second_b, at_y(-1))
    y1["a", 1, 2] = message(second_a, second_a, at_y(1))
    y1["a", -1, 2] = message(first_a, first_a, at_y(-1))
    y1["b", 1, 2] = message(second_b, second_b, at_y(1))
    y1["b", -1, 2] = message(first_b, first_b, at_y(-1))
    gain0[:, :CA] = gain_a
    gain0[:, CA:] = gain_b
    gain_c = message(gain0, gain0_rec, c_peer)
    out_gr = fetch(gr, gr_hbm)

    def block_at(zz, step):
        return zz * 4 + (y + step) % 4

    def forward_on(buf, zz, sent, key):
        sent[key, 1, 1].wait_recv()
        part = buf.at[block_at(zz, -1), first]
        sent[key, 1, 3] = message(part, part, at_y(1))
        sent[key, -1, 1].wait_recv()
        part = buf.at[block_at(zz, 1), second]
        sent[key, -1, 3] = message(part, part, at_y(-1))

    def across(step):
        part = all_a.at[block_at(z, step)]
        zx_a[step] = message(part, part, z_peer)

    def accumulate(blocks, start):
        def one(j, carry):
            block = blocks(j)
            grad = jnp.concatenate([all_a[block], all_b[block]], axis=1)
            r = dot(grad, w[w_rows(block), :], 1, 0)
            if start:
                gacc[...] = r
            else:
                gacc[...] += r
            return carry

        lax.fori_loop(0, 1 if start else 2, one, 0)

    def group_of(g):
        zz = z if g < 2 else 1 - z
        pair = y // 2 if g % 2 == 0 else 1 - y // 2
        return zz * 2 + pair

    cx = {}

    def weight_grad(g):
        kk = group_of(g)

        def one(j, carry):
            block = kk * 2 + j
            grad = jnp.concatenate([all_a[block], all_b[block]], axis=1)
            r = dot(grad, att[...], 0, 0).astype(BF16)
            for s in range(4):
                gwb[g, s % 2, 2 * j + s // 2] = r[s * OUT_ROWS : (s + 1) * OUT_ROWS]
            return carry

        lax.fori_loop(0, 2, one, 0)
        cx[g] = message(gwb.at[g, 1 - c], cx_rec.at[g], c_peer)

    low_rows, high_rows = pl.ds(0, HALF_ROWS), pl.ds(HALF_ROWS, HALF_ROWS)
    xs = {}

    def x_first(g):
        cx[g].wait_recv()

        def u_of(d):
            to = (x + d) % 4
            u[g, d] = gwb[g, c, to] + cx_rec[g, to]

        u_of(2)
        xs[g, 1, 1] = message(u.at[g, 2, low_rows], x_rec.at[g, 0], at_x(1))
        xs[g, -1, 1] = message(u.at[g, 2, high_rows], x_rec.at[g, 1], at_x(-1))
        u_of(1)
        xs[g, 1, 2] = message(u.at[g, 1, high_rows], x_rec.at[g, 2], at_x(1))
        u_of(3)
        xs[g, -1, 2] = message(u.at[g, 3, low_rows], x_rec.at[g, 3], at_x(-1))
        u_of(0)

    def x_second(g):
        xs[g, 1, 1].wait_recv()
        x_mer[g, 0] = u[g, 1, :HALF_ROWS] + x_rec[g, 0]
        xs[g, 1, 3] = message(x_mer.at[g, 0], x_rec.at[g, 4], at_x(1))
        xs[g, -1, 1].wait_recv()
        x_mer[g, 1] = u[g, 3, HALF_ROWS:] + x_rec[g, 1]
        xs[g, -1, 3] = message(x_mer.at[g, 1], x_rec.at[g, 5], at_x(-1))

    zs = {}

    def z_copy(g):
        kk = group_of(g)
        d = (kk - zh) % 4
        slot = (d + 3) % 4
        return d, pltpu.make_async_remote_copy(
            src_ref=z_send.at[g], dst_ref=z_rec.at[slot],
            send_sem=ssem.at[MESSAGES - 4 + g], recv_sem=rsem.at[MESSAGES - 4 + slot],
            device_id={"dp": kk * 8 + x * 2 + c}, device_id_type=MESH,
        )

    def x_last(g):
        for step in (1, -1):
            xs[g, step, 2].wait_recv()
            xs[g, step, 3].wait_recv()
        upper = u[g, 0, :HALF_ROWS].astype(F32) + x_rec[g, 3].astype(F32) + x_rec[g, 4].astype(F32)
        lower = u[g, 0, HALF_ROWS:].astype(F32) + x_rec[g, 2].astype(F32) + x_rec[g, 5].astype(F32)
        z_send[g, :HALF_ROWS] = upper.astype(BF16)
        z_send[g, HALF_ROWS:] = lower.astype(BF16)
        d, copy = z_copy(g)

        @pl.when(d != 0)
        def _():
            copy.start()

        @pl.when(d == 0)
        def _():
            z_own[:HALF_ROWS] = upper
            z_own[HALF_ROWS:] = lower

    accumulate(lambda j: t, True)
    forward_on(all_a, z, y1, "a")
    forward_on(all_b, z, y1, "b")
    zx_b.wait_recv()
    y2 = {}
    other = block_at(1 - z, 0)
    first_p = all_b.at[other, first]
    second_p = all_b.at[other, second]
    y2["b", 1, 1] = message(first_p, first_p, at_y(1))
    y2["b", -1, 1] = message(second_p, second_p, at_y(-1))
    y2["b", 1, 2] = message(second_p, second_p, at_y(1))
    y2["b", -1, 2] = message(first_p, first_p, at_y(-1))
    y1["a", 1, 2].wait_recv()
    across(-1)
    y1["a", -1, 2].wait_recv()
    across(1)
    gain_c.wait_recv()
    gain1[...] = gain0[...] + gain0_rec[...]
    gain_x = [message(gain1, gain1_rec.at[s - 1], at_x(s)) for s in (1, 2, 3)]
    y1["b", 1, 2].wait_recv()
    y1["b", -1, 2].wait_recv()
    weight_grad(0)
    x_first(0)
    y1["a", 1, 3].wait_recv()
    y1["a", -1, 3].wait_recv()
    across(2)
    accumulate(lambda j: block_at(z, 1) * j + block_at(z, -1) * (1 - j), False)
    x_second(0)
    y1["b", 1, 3].wait_recv()
    y1["b", -1, 3].wait_recv()
    weight_grad(1)
    x_first(1)
    x_second(1)
    forward_on(all_b, 1 - z, y2, "b")
    zx_a[0].wait_recv()
    accumulate(lambda j: block_at(z, 2) * j + block_at(1 - z, 0) * (1 - j), False)
    for copy in gain_x:
        copy.wait_recv()
    gain2[...] = gain1[...] + gain1_rec[0] + gain1_rec[1] + gain1_rec[2]
    gain_z = [message(gain2, gain2_rec.at[s - 1], at_zh(s)) for s in (1, 2, 3)]
    x_last(0)
    zx_a[-1].wait_recv()
    zx_a[1].wait_recv()
    y2["b", 1, 2].wait_recv()
    y2["b", -1, 2].wait_recv()
    weight_grad(2)
    x_first(2)
    accumulate(lambda j: block_at(1 - z, 1) * j + block_at(1 - z, -1) * (1 - j), False)
    zx_a[2].wait_recv()
    y2["b", 1, 3].wait_recv()
    y2["b", -1, 3].wait_recv()
    weight_grad(3)
    x_first(3)
    x_second(2)
    last = block_at(1 - z, 2)
    grad = jnp.concatenate([all_a[last], all_b[last]], axis=1)
    ga[...] = (gacc[...] + dot(grad, w[w_rows(last), :], 1, 0)).astype(BF16)
    x_last(1)

    def backward(h, carry):
        cols = head_cols(h)
        g_head = ga[:, cols]
        p = probs[h]
        gv[:, cols] = dot(p.astype(BF16), g_head, 0, 0).astype(BF16)
        gp = dot(g_head, v[:, cols], 1, 1)
        delta = jnp.sum(p * gp, axis=1, keepdims=True)
        gs = (p * (gp - delta) * SCALE).astype(BF16)
        gq[:, cols] = dot(gs, k[:, cols], 1, 0).astype(BF16)
        gk[:, cols] = dot(gs, q[:, cols], 0, 0).astype(BF16)
        return carry

    lax.fori_loop(0, 2, backward, 0)
    x_second(3)
    lax.fori_loop(2, 4, backward, 0)
    x_last(2)
    lax.fori_loop(4, HEADS, backward, 0)
    out_gq, out_gk, out_gv = fetch(gq, gq_hbm), fetch(gk, gk_hbm), fetch(gv, gv_hbm)
    for copy in gain_z:
        copy.wait_recv()
    gain = gain2[...] + gain2_rec[0] + gain2_rec[1] + gain2_rec[2]
    gg_ref[...] = jnp.sum(gain, axis=0, keepdims=True)
    x_last(3)

    for slot in range(3):
        pltpu.make_async_remote_copy(
            src_ref=z_send.at[0], dst_ref=z_rec.at[slot],
            send_sem=ssem.at[MESSAGES - 4], recv_sem=rsem.at[MESSAGES - 4 + slot],
            device_id=c_peer, device_id_type=MESH,
        ).wait_recv()
    gw_out[...] = (
        z_own[...] + z_rec[0].astype(F32) + z_rec[1].astype(F32) + z_rec[2].astype(F32)
    )
    out_gw = fetch(gw_out, gw_hbm)

    for copy in messages:
        copy.wait_send()
    for g in range(4):
        d, copy = z_copy(g)

        @pl.when(d != 0)
        def _():
            copy.wait_send()

    for copy in (out_lo, out_gr, out_gq, out_gk, out_gv, out_gw):
        copy.wait()
    assert len(messages) <= MESSAGES - 4


def shards(q, k, v, mask, res, w, gain, ups, rg):
    rows = jax.ShapeDtypeStruct((LEN, WIDTH), BF16)
    anywhere = pl.BlockSpec(memory_space=pl.ANY)
    vmem = pl.BlockSpec(memory_space=pltpu.VMEM)

    def b(*shape):
        return pltpu.VMEM(shape, BF16)

    def f(*shape):
        return pltpu.VMEM(shape, F32)

    slab = (LEN, WIDTH)
    part = (OUT_ROWS, WIDTH)
    half = (HALF_ROWS, WIDTH)
    scratch = [
        b(*slab), b(*slab), b(*slab), b(*slab), b(D, WIDTH), b(*slab), b(*slab),
        f(LEN, LEN), f(HEADS, LEN, LEN), b(*slab), b(*slab), b(*slab), b(*slab), f(*slab),
        b(*slab), b(*slab), b(*slab), f(*part),
        b(4, 2, LEN, CA), b(4, 2, LEN, CB), b(4, LEN, CA), b(6, HALF, CA), b(6, 2, HALF, CB),
        b(2, HALF, CA), b(2, 2, HALF, CB), b(LEN, CB), b(LEN, CB), f(*slab),
        f(8, LEN), f(8, 8, LEN), b(8, LEN, CA), b(8, LEN, CB),
        b(4, 2, 4, *part), b(4, 4, *part), b(4, 4, *part), b(4, 6, *half), b(4, 2, *half),
        b(4, *part), b(4, *part), f(*part),
        f(8, WIDTH), f(8, WIDTH), f(8, WIDTH), f(3, 8, WIDTH), f(8, WIDTH), f(3, 8, WIDTH),
        pltpu.SemaphoreType.DMA((MESSAGES,)),
        pltpu.SemaphoreType.DMA((MESSAGES,)),
        pltpu.SemaphoreType.DMA((16,)),
    ]
    outs = pl.pallas_call(
        kernel,
        out_shape=(
            rows, rows, rows, rows, rows,
            jax.ShapeDtypeStruct(part, F32),
            jax.ShapeDtypeStruct((1, WIDTH), F32),
        ),
        in_specs=[anywhere, anywhere, anywhere, vmem, anywhere, anywhere, vmem, anywhere, anywhere],
        out_specs=(anywhere,) * 6 + (vmem,),
        scratch_shapes=scratch,
        compiler_params=pltpu.CompilerParams(
            collective_id=0, has_side_effects=True, vmem_limit_bytes=64000000
        ),
    )(q, k, v, mask, res, w, gain.reshape(1, WIDTH), ups, rg)
    return (*outs[:6], outs[6].reshape(WIDTH))


def solution(mesh):
    placed = P("dp", "tensor")
    return jax.shard_map(
        shards,
        mesh=mesh,
        in_specs=(placed, placed, placed, P("dp", None), placed, P(None, "tensor"), P("tensor"), placed, placed),
        out_specs=(placed,) * 6 + (P("tensor"),),
        check_vma=False,
    )
```

```python
import functools

import jax
import jax.numpy as jnp
from jax import lax
from jax.experimental import pallas as pl
from jax.experimental.pallas import tpu as pltpu
from jax.sharding import PartitionSpec as P

MESH = pl.DeviceIdType.MESH
F32 = jnp.float32
BF16 = jnp.bfloat16

D = 5120
HEAD_DIM = 128
LEN = 384
WIDTH = 640
HEADS = WIDTH // HEAD_DIM
CA = 256
CB = WIDTH - CA
HALF = LEN // 2
OUT_ROWS = 160
HALF_ROWS = OUT_ROWS // 2
SCALE = HEAD_DIM ** (-0.5)
EPSILON = 1e-05
MESSAGES = 128
VMEM_LIMIT = 51 << 20


def dot(a, b, ca, cb):
    return lax.dot_general(a, b, (((ca,), (cb,)), ((), ())), preferred_element_type=F32)


def kernel(
    q_hbm, k_hbm, v_hbm, mask_hbm, res_hbm, w_hbm, gain_hbm, ups_hbm, rg_hbm,
    lo, gr, gq, gk, gv, gw_out, gg_ref,
    q, k, v, mask_ref, res, w, gain_ref, ups, rg, bias, probs, att, ga, gacc,
    pa, pb, rec_az, rec_a, rec_b, mer_a, mer_b, zb_send, zb_rec, own,
    stat, stat_rec, all_a, all_b,
    gwb, cx_rec, u, x_rec, x_mer, z_send, z_rec, z_mer, z_own,
    gain0, gain0_rec, gain1, gain1_rec, gain2, gain2_rec,
    ssem, rsem, lsem,
):
    t = lax.axis_index("tensor")
    dp = lax.axis_index("dp")
    z, y = t // 4, t % 4
    c, x, zh = dp % 2, (dp // 2) % 4, dp // 8

    def at_y(step):
        return {"tensor": z * 4 + (y + step) % 4}

    z_peer = {"tensor": (1 - z) * 4 + y}
    c_peer = {"dp": dp + 1 - 2 * c}

    def at_x(step):
        return {"dp": zh * 8 + ((x + step) % 4) * 2 + c}

    def at_zh(step):
        return {"dp": ((zh + step) % 4) * 8 + x * 2 + c}

    peers = [{"tensor": (t + j) % 8} for j in range(1, 8)]
    peers += [c_peer]
    peers += [at_x(s) for s in (1, 2, 3)]
    peers += [at_zh(s) for s in (1, 2, 3)]

    local = []

    def fetch(src, dst):
        copy = pltpu.make_async_copy(src, dst, lsem.at[len(local)])
        local.append(copy)
        copy.start()
        return copy

    in_mask = fetch(mask_hbm, mask_ref)
    in_q, in_k, in_v = fetch(q_hbm, q), fetch(k_hbm, k), fetch(v_hbm, v)
    in_w = fetch(w_hbm, w)
    in_gain = fetch(gain_hbm, gain_ref)
    in_res, in_ups, in_rg = fetch(res_hbm, res), fetch(ups_hbm, ups), fetch(rg_hbm, rg)

    barrier = pltpu.get_barrier_semaphore()
    for peer in peers:
        pl.semaphore_signal(barrier, inc=1, device_id=peer, device_id_type=MESH)

    messages = []

    def message(src, dst, device, start=True):
        i = len(messages)
        copy = pltpu.make_async_remote_copy(
            src_ref=src, dst_ref=dst, send_sem=ssem.at[i], recv_sem=rsem.at[i],
            device_id=device, device_id_type=MESH,
        )
        messages.append(copy)
        if start:
            copy.start()
        return copy

    in_mask.wait()
    zeros = jnp.sum(1 - mask_ref[...], axis=1, keepdims=True)
    row = lax.broadcasted_iota(jnp.int32, (LEN, LEN), 0)
    col = lax.broadcasted_iota(jnp.int32, (LEN, LEN), 1)
    allowed = (col <= row) | (jnp.maximum(row, col) < zeros)
    bias[...] = jnp.where(allowed, 0.0, -jnp.inf).astype(F32)
    in_q.wait()
    in_k.wait()
    in_v.wait()

    def head_cols(h):
        return pl.ds(pl.multiple_of(h * HEAD_DIM, HEAD_DIM), HEAD_DIM)

    def forward(h, carry):
        cols = head_cols(h)
        s = dot(q[:, cols], k[:, cols], 1, 1) * SCALE + bias[...]
        e = jnp.exp(s - jnp.max(s, axis=1, keepdims=True))
        p = e * (1.0 / jnp.sum(e, axis=1, keepdims=True))
        probs[h] = p
        att[:, cols] = dot(p.astype(BF16), v[:, cols], 1, 0).astype(BF16)
        return carry

    lax.fori_loop(0, HEADS, forward, 0)
    in_w.wait()

    def w_rows(block):
        return pl.ds(pl.multiple_of(block * WIDTH, WIDTH), WIDTH)

    def project(d):
        def one(j, carry):
            zz = j * z + (1 - j) * (1 - z)
            block = zz * 4 + (y + d) % 4
            r = dot(att[...], w[w_rows(block), :], 1, 1)
            pa[d, j] = r[:, :CA].astype(BF16)
            pb[d, zz] = r[:, CA:].astype(BF16)
            return carry

        lax.fori_loop(0, 2, one, 0)

    first, second = pl.ds(0, HALF), pl.ds(HALF, HALF)
    az, b1, b2, a1, a2 = {}, {}, {}, {}, {}
    project(2)
    pl.semaphore_wait(barrier, len(peers))
    b1[1] = message(pb.at[2, :, first], rec_b.at[0], at_y(1))
    b1[-1] = message(pb.at[2, :, second], rec_b.at[1], at_y(-1))
    az[2] = message(pa.at[2, 0], rec_az.at[2], z_peer)
    project(1)
    b2[1] = message(pb.at[1, :, second], rec_b.at[2], at_y(1))
    az[1] = message(pa.at[1, 0], rec_az.at[1], z_peer)
    project(3)
    b2[-1] = message(pb.at[3, :, first], rec_b.at[3], at_y(-1))
    az[3] = message(pa.at[3, 0], rec_az.at[3], z_peer)
    project(0)
    az[0] = message(pa.at[0, 0], rec_az.at[0], z_peer)

    b1[1].wait_recv()
    mer_b[0] = pb[1, :, :HALF] + rec_b[0]
    b3 = {1: message(mer_b.at[0], rec_b.at[4], at_y(1))}
    b1[-1].wait_recv()
    mer_b[1] = pb[3, :, HALF:] + rec_b[1]
    b3[-1] = message(mer_b.at[1], rec_b.at[5], at_y(-1))

    def join(d):
        az[d].wait_recv()
        pa[d, 1] = pa[d, 1] + rec_az[d]

    join(2)
    a1[1] = message(pa.at[2, 1, first], rec_a.at[0], at_y(1))
    a1[-1] = message(pa.at[2, 1, second], rec_a.at[1], at_y(-1))
    join(1)
    a2[1] = message(pa.at[1, 1, second], rec_a.at[2], at_y(1))
    join(3)
    a2[-1] = message(pa.at[3, 1, first], rec_a.at[3], at_y(-1))
    az[0].wait_recv()

    b2[1].wait_recv()
    b2[-1].wait_recv()
    b3[1].wait_recv()
    b3[-1].wait_recv()

    def b_sum(zz):
        top = pb[0, zz, :HALF].astype(F32) + rec_b[3, zz].astype(F32) + rec_b[4, zz].astype(F32)
        low = pb[0, zz, HALF:].astype(F32) + rec_b[2, zz].astype(F32) + rec_b[5, zz].astype(F32)
        return top, low

    top, low = b_sum(1 - z)
    zb_send[:HALF] = top.astype(BF16)
    zb_send[HALF:] = low.astype(BF16)
    zb = message(zb_send, zb_rec, z_peer)

    a1[1].wait_recv()
    mer_a[0] = pa[1, 1, :HALF] + rec_a[0]
    a3 = {1: message(mer_a.at[0], rec_a.at[4], at_y(1))}
    a1[-1].wait_recv()
    mer_a[1] = pa[3, 1, HALF:] + rec_a[1]
    a3[-1] = message(mer_a.at[1], rec_a.at[5], at_y(-1))

    in_res.wait()
    in_ups.wait()
    in_gain.wait()
    gain_row = gain_ref[...].reshape(1, WIDTH)
    in_rg.wait()
    top, low = b_sum(z)
    own[:HALF, CA:] = top
    own[HALF:, CA:] = low
    own[:, :CA] = pa[0, 1].astype(F32) + rec_az[0].astype(F32)

    zb.wait_recv()
    own_b = own[:, CA:] + zb_rec[...].astype(F32) + res[:, CA:].astype(F32)
    low_b = own_b.astype(BF16)
    lo[:, CA:] = low_b
    f_b = low_b.astype(F32)
    scaled_b = ups[:, CA:].astype(F32) * gain_row[:, CA:]
    square = jnp.sum(f_b * f_b, axis=1, keepdims=True)
    inner = jnp.sum(f_b * scaled_b, axis=1, keepdims=True)

    a2[1].wait_recv()
    a2[-1].wait_recv()
    a3[1].wait_recv()
    a3[-1].wait_recv()
    top = own[:HALF, :CA] + rec_a[3].astype(F32) + rec_a[4].astype(F32) + res[:HALF, :CA].astype(F32)
    low = own[HALF:, :CA] + rec_a[2].astype(F32) + rec_a[5].astype(F32) + res[HALF:, :CA].astype(F32)
    lo[:HALF, :CA] = top.astype(BF16)
    lo[HALF:, :CA] = low.astype(BF16)
    f_a = lo[:, :CA].astype(F32)
    scaled_a = ups[:, :CA].astype(F32) * gain_row[:, :CA]
    square = square + jnp.sum(f_a * f_a, axis=1, keepdims=True)
    inner = inner + jnp.sum(f_a * scaled_a, axis=1, keepdims=True)

    lane = lax.broadcasted_iota(jnp.int32, (LEN, 128), 1)
    packed = jnp.where(lane == 0, square, jnp.where(lane == 1, inner, 0.0))
    stat[...] = packed.T[:8]
    stats = [message(stat, stat_rec.at[j], peers[j - 1]) for j in range(1, 8)]
    total = stat[...]
    for j in range(1, 8):
        stats[j - 1].wait_recv()
        total = total + stat_rec[j]
    wide = jnp.concatenate([total, jnp.zeros((120, LEN), F32)], axis=0).T
    square, inner = wide[:, 0:1], wide[:, 1:2]
    rms = jnp.sqrt(square / D + EPSILON)
    back = 1.0 / rms
    row_inner = inner / (rms * D)

    def grad_rows(lo_part, ups_part, gain_part, rg_part):
        up = ups_part.astype(F32)
        normed = lo_part.astype(F32) * back
        g = rg_part.astype(F32) + (up * gain_part - normed * row_inner) * back
        return g.astype(BF16), (up * normed).reshape(LEN // 8, 8, -1).sum(axis=0)

    g, gain_a = grad_rows(lo[:, :CA], ups[:, :CA], gain_row[:, :CA], rg[:, :CA])
    all_a[t] = g
    gr[:, :CA] = g
    mine_a = all_a.at[t]
    first_a = all_a.at[t, first]
    second_a = all_a.at[t, second]
    y1 = {}
    y1["a", 1, 1] = message(first_a, first_a, at_y(1))
    y1["a", -1, 1] = message(second_a, second_a, at_y(-1))
    g, gain_b = grad_rows(lo[:, CA:], ups[:, CA:], gain_row[:, CA:], rg[:, CA:])
    all_b[t] = g
    gr[:, CA:] = g
    zx_b = message(all_b.at[t], all_b.at[t], z_peer)
    zx_a = {0: message(mine_a, mine_a, z_peer)}
    first_b = all_b.at[t, first]
    second_b = all_b.at[t, second]
    y1["b", 1, 1] = message(first_b, first_b, at_y(1))
    y1["b", -1, 1] = message(second_b, second_b, at_y(-1))
    y1["a", 1, 2] = message(second_a, second_a, at_y(1))
    y1["a", -1, 2] = message(first_a, first_a, at_y(-1))
    y1["b", 1, 2] = message(second_b, second_b, at_y(1))
    y1["b", -1, 2] = message(first_b, first_b, at_y(-1))
    gain0[:, :CA] = gain_a
    gain0[:, CA:] = gain_b
    gain_c = message(gain0, gain0_rec, c_peer)

    def block_at(zz, step):
        return zz * 4 + (y + step) % 4

    def forward_on(buf, zz, sent, key):
        sent[key, 1, 1].wait_recv()
        part = buf.at[block_at(zz, -1), first]
        sent[key, 1, 3] = message(part, part, at_y(1))
        sent[key, -1, 1].wait_recv()
        part = buf.at[block_at(zz, 1), second]
        sent[key, -1, 3] = message(part, part, at_y(-1))

    def across(step):
        part = all_a.at[block_at(z, step)]
        zx_a[step] = message(part, part, z_peer)

    def accumulate(blocks, start):
        def one(j, carry):
            block = blocks(j)
            grad = jnp.concatenate([all_a[block], all_b[block]], axis=1)
            r = dot(grad, w[w_rows(block), :], 1, 0)
            if start:
                gacc[...] = r
            else:
                gacc[...] += r
            return carry

        lax.fori_loop(0, 1 if start else 2, one, 0)

    order = [t, block_at(1 - z, 0), block_at(z, -1), block_at(z, 1), block_at(z, 2)]
    order += [block_at(1 - z, -1), block_at(1 - z, 1), block_at(1 - z, 2)]
    cx = {}

    def weight_grad(i):
        grad = jnp.concatenate([all_a[order[i]], all_b[order[i]]], axis=1)
        r = dot(grad, att[...], 0, 0).astype(BF16)
        for s in range(4):
            gwb[i, s % 2, s // 2] = r[s * OUT_ROWS : (s + 1) * OUT_ROWS]
        cx[i] = message(gwb.at[i, 1 - c], cx_rec.at[i], c_peer)

    low_rows, high_rows = pl.ds(0, HALF_ROWS), pl.ds(HALF_ROWS, HALF_ROWS)
    waits = []

    def has(i, d):
        return (x + d) % 4 // 2 == order[i] % 2

    def start_when(condition, *made):
        waits.extend((condition, make) for make in made)
        for make in made:
            make().start()

    X_SEM, Z_SEM = MESSAGES, MESSAGES + 48

    def x_copy(i, kind, src, step):
        sem = X_SEM + 6 * i + kind
        return pltpu.make_async_remote_copy(
            src_ref=src, dst_ref=x_rec.at[i, kind], send_sem=ssem.at[sem], recv_sem=rsem.at[sem],
            device_id=at_x(step), device_id_type=MESH,
        )

    def x_far(i, src, step):
        sem = X_SEM + 6 * i
        return pltpu.make_async_remote_copy(
            src_ref=src, dst_ref=x_rec.at[i, 0], send_sem=ssem.at[sem + (5 if step < 0 else 0)],
            recv_sem=rsem.at[sem], device_id=at_x(step), device_id_type=MESH,
        )

    def z_copy(kind, src, step):
        sem = Z_SEM + kind
        return pltpu.make_async_remote_copy(
            src_ref=src, dst_ref=z_rec.at[kind], send_sem=ssem.at[sem], recv_sem=rsem.at[sem],
            device_id=at_zh(step), device_id_type=MESH,
        )

    def x_first(i):
        cx[i].wait_recv()
        u[i] = gwb[i, c] + cx_rec[i]
        far, near, back_near = (x + 2) % 2, (x + 1) % 2, (x + 3) % 2
        is_far, is_next, is_back = has(i, 2), has(i, 1), has(i, 3)

        @pl.when(is_far)
        def _():
            start_when(
                is_far,
                lambda: x_far(i, u.at[i, far, low_rows], 1),
                lambda: x_far(i, u.at[i, far, high_rows], -1),
            )

        @pl.when(is_next)
        def _():
            start_when(is_next, lambda: x_copy(i, 1, u.at[i, near, high_rows], 1))

        @pl.when(is_back)
        def _():
            start_when(is_back, lambda: x_copy(i, 3, u.at[i, back_near, low_rows], -1))

    def x_second(i):
        near, back_near = (x + 1) % 2, (x + 3) % 2
        is_next, is_back = has(i, 1), has(i, 3)

        @pl.when(is_next)
        def _():
            x_far(i, x_mer.at[i], 1).wait_recv()
            x_mer[i] = u[i, near, :HALF_ROWS] + x_rec[i, 0]
            start_when(is_next, lambda: x_copy(i, 2, x_mer.at[i], 1))

        @pl.when(is_back)
        def _():
            x_far(i, x_mer.at[i], -1).wait_recv()
            x_mer[i] = u[i, back_near, HALF_ROWS:] + x_rec[i, 0]
            start_when(is_back, lambda: x_copy(i, 4, x_mer.at[i], -1))

    def x_last(i):
        kk = order[i] // 2
        e = (kk - zh) % 4
        mine = has(i, 0)
        is_far, is_next, is_back = mine & (e == 2), mine & (e == 1), mine & (e == 3)

        @pl.when(mine)
        def _():
            for kind in (1, 2, 3, 4):
                x_copy(i, kind, x_mer.at[i], 1).wait_recv()
            upper = u[i, x % 2, :HALF_ROWS].astype(F32) + x_rec[i, 2].astype(F32) + x_rec[i, 3].astype(F32)
            lower = u[i, x % 2, HALF_ROWS:].astype(F32) + x_rec[i, 1].astype(F32) + x_rec[i, 4].astype(F32)
            z_send[i, :HALF_ROWS] = upper.astype(BF16)
            z_send[i, HALF_ROWS:] = lower.astype(BF16)

            @pl.when(e == 0)
            def _():
                z_own[:HALF_ROWS] = upper
                z_own[HALF_ROWS:] = lower

        @pl.when(is_far)
        def _():
            start_when(
                is_far,
                lambda: z_copy(0, z_send.at[i, low_rows], 1),
                lambda: z_copy(1, z_send.at[i, high_rows], -1),
            )

        @pl.when(is_next)
        def _():
            start_when(is_next, lambda: z_copy(2, z_send.at[i, high_rows], 1))

        @pl.when(is_back)
        def _():
            start_when(is_back, lambda: z_copy(4, z_send.at[i, low_rows], -1))

    def z_second(i):
        e = (order[i] // 2 - zh) % 4
        is_next, is_back = has(i, 0) & (e == 1), has(i, 0) & (e == 3)

        @pl.when(is_next)
        def _():
            z_copy(0, z_mer.at[0], 1).wait_recv()
            z_mer[0] = z_send[i, :HALF_ROWS] + z_rec[0]
            start_when(is_next, lambda: z_copy(3, z_mer.at[0], 1))

        @pl.when(is_back)
        def _():
            z_copy(1, z_mer.at[1], -1).wait_recv()
            z_mer[1] = z_send[i, HALF_ROWS:] + z_rec[1]
            start_when(is_back, lambda: z_copy(5, z_mer.at[1], -1))

    weight_grad(0)
    accumulate(lambda j: t, True)
    forward_on(all_a, z, y1, "a")
    forward_on(all_b, z, y1, "b")
    zx_b.wait_recv()
    y2 = {}
    other = block_at(1 - z, 0)
    first_p = all_b.at[other, first]
    second_p = all_b.at[other, second]
    y2["b", 1, 1] = message(first_p, first_p, at_y(1))
    y2["b", -1, 1] = message(second_p, second_p, at_y(-1))
    y2["b", 1, 2] = message(second_p, second_p, at_y(1))
    y2["b", -1, 2] = message(first_p, first_p, at_y(-1))
    x_first(0)
    y1["a", 1, 2].wait_recv()
    across(-1)
    y1["a", -1, 2].wait_recv()
    across(1)
    zx_a[0].wait_recv()
    weight_grad(1)
    gain_c.wait_recv()
    gain1[...] = gain0[...] + gain0_rec[...]
    gain_x = [message(gain1, gain1_rec.at[s - 1], at_x(s)) for s in (1, 2, 3)]
    y1["b", 1, 2].wait_recv()
    y1["b", -1, 2].wait_recv()
    weight_grad(2)
    weight_grad(3)
    x_second(0)
    x_first(1)
    y1["a", 1, 3].wait_recv()
    y1["a", -1, 3].wait_recv()
    across(2)
    accumulate(lambda j: order[3] * j + order[2] * (1 - j), False)
    x_second(1)
    x_first(2)
    x_first(3)
    y1["b", 1, 3].wait_recv()
    y1["b", -1, 3].wait_recv()
    weight_grad(4)
    x_last(0)
    accumulate(lambda j: order[4] * j + order[1] * (1 - j), False)
    forward_on(all_b, 1 - z, y2, "b")
    x_second(2)
    x_second(3)
    x_first(4)
    x_last(1)
    z_second(0)
    for copy in gain_x:
        copy.wait_recv()
    gain2[...] = gain1[...] + gain1_rec[0] + gain1_rec[1] + gain1_rec[2]
    gain_z = [message(gain2, gain2_rec.at[s - 1], at_zh(s)) for s in (1, 2, 3)]
    zx_a[-1].wait_recv()
    zx_a[1].wait_recv()
    y2["b", 1, 2].wait_recv()
    y2["b", -1, 2].wait_recv()
    weight_grad(5)
    weight_grad(6)
    x_second(4)
    x_last(2)
    z_second(1)
    zx_a[2].wait_recv()
    y2["b", 1, 3].wait_recv()
    y2["b", -1, 3].wait_recv()
    weight_grad(7)
    x_first(5)
    x_first(6)
    x_last(3)
    accumulate(lambda j: order[6] * j + order[5] * (1 - j), False)
    x_first(7)
    x_second(5)
    x_second(6)
    x_last(4)
    z_second(2)
    z_second(3)
    last = order[7]
    grad = jnp.concatenate([all_a[last], all_b[last]], axis=1)
    ga[...] = (gacc[...] + dot(grad, w[w_rows(last), :], 1, 0)).astype(BF16)
    x_second(7)

    def backward(h, carry):
        cols = head_cols(h)
        g_head = ga[:, cols]
        p = probs[h]
        gv[:, cols] = dot(p.astype(BF16), g_head, 0, 0).astype(BF16)
        gp = dot(g_head, v[:, cols], 1, 1)
        delta = jnp.sum(p * gp, axis=1, keepdims=True)
        gs = (p * (gp - delta) * SCALE).astype(BF16)
        gq[:, cols] = dot(gs, k[:, cols], 1, 0).astype(BF16)
        gk[:, cols] = dot(gs, q[:, cols], 0, 0).astype(BF16)
        return carry

    lax.fori_loop(0, 2, backward, 0)
    x_last(5)
    z_second(4)
    lax.fori_loop(2, 4, backward, 0)
    x_last(6)
    z_second(5)
    lax.fori_loop(4, HEADS, backward, 0)
    for copy in gain_z:
        copy.wait_recv()
    gain = gain2[...] + gain2_rec[0] + gain2_rec[1] + gain2_rec[2]
    gg_ref[...] = jnp.sum(gain, axis=0)
    x_last(7)
    z_second(6)
    z_second(7)

    for kind in (2, 3, 4, 5):
        z_copy(kind, z_mer.at[0], 1).wait_recv()
    gw_out[:HALF_ROWS] = z_own[:HALF_ROWS] + z_rec[3].astype(F32) + z_rec[4].astype(F32)
    gw_out[HALF_ROWS:] = z_own[HALF_ROWS:] + z_rec[2].astype(F32) + z_rec[5].astype(F32)

    for copy in messages:
        copy.wait_send()
    for condition, make in waits:

        @pl.when(condition)
        def _():
            make().wait_send()

    assert len(messages) <= MESSAGES


def hand_over(*refs):
    n = len(refs) // 2
    sources, outs, sems = refs[:n], refs[n : 2 * n], refs[2 * n]
    copies = [pltpu.make_async_copy(a, b, sems.at[i]) for i, (a, b) in enumerate(zip(sources, outs))]
    for copy in copies:
        copy.start()
    for copy in copies:
        copy.wait()


def deliver(arrays):
    vmem = pl.BlockSpec(memory_space=pltpu.VMEM)
    return pl.pallas_call(
        hand_over,
        out_shape=[jax.ShapeDtypeStruct(a.shape, a.dtype) for a in arrays],
        in_specs=[vmem] * len(arrays),
        out_specs=[pl.BlockSpec(memory_space=pl.ANY)] * len(arrays),
        scratch_shapes=[pltpu.SemaphoreType.DMA((len(arrays),))],
        compiler_params=pltpu.CompilerParams(vmem_limit_bytes=8 << 20),
    )(*arrays)


def shards(q, k, v, mask, res, w, gain, ups, rg):
    rows = jax.ShapeDtypeStruct((LEN, WIDTH), BF16)
    hbm = pl.BlockSpec(memory_space=pltpu.HBM)
    vmem = pl.BlockSpec(memory_space=pltpu.VMEM)

    def b(*shape):
        return pltpu.VMEM(shape, BF16)

    def f(*shape):
        return pltpu.VMEM(shape, F32)

    slab = (LEN, WIDTH)
    part = (OUT_ROWS, WIDTH)
    half = (HALF_ROWS, WIDTH)
    scratch = [
        b(*slab), b(*slab), b(*slab), pltpu.VMEM((1, LEN), jnp.int32), b(*slab), b(D, WIDTH), f(WIDTH), b(*slab), b(*slab),
        f(LEN, LEN), f(HEADS, LEN, LEN), b(*slab), b(*slab), f(*slab),
        b(4, 2, LEN, CA), b(4, 2, LEN, CB), b(4, LEN, CA), b(6, HALF, CA), b(6, 2, HALF, CB),
        b(2, HALF, CA), b(2, 2, HALF, CB), b(LEN, CB), b(LEN, CB), f(*slab),
        f(8, LEN), f(8, 8, LEN), b(8, LEN, CA), b(8, LEN, CB),
        b(8, 2, 2, *part), b(8, 2, *part), b(8, 2, *part), b(8, 5, *half), b(8, *half),
        b(8, *part), b(6, *half), b(2, *half), f(*part),
        f(8, WIDTH), f(8, WIDTH), f(8, WIDTH), f(3, 8, WIDTH), f(8, WIDTH), f(3, 8, WIDTH),
        pltpu.SemaphoreType.DMA((MESSAGES + 54,)),
        pltpu.SemaphoreType.DMA((MESSAGES + 54,)),
        pltpu.SemaphoreType.DMA((16,)),
    ]
    outs = pl.pallas_call(
        kernel,
        out_shape=(
            rows, rows, rows, rows, rows,
            jax.ShapeDtypeStruct(part, F32),
            jax.ShapeDtypeStruct((WIDTH,), F32),
        ),
        in_specs=[hbm] * 9,
        out_specs=(vmem,) * 7,
        scratch_shapes=scratch,
        compiler_params=pltpu.CompilerParams(
            collective_id=0, has_side_effects=True, vmem_limit_bytes=VMEM_LIMIT
        ),
    )(q, k, v, mask, res, w, gain, ups, rg)
    return deliver(outs)


def solution(mesh):
    placed = P("dp", "tensor")
    return jax.shard_map(
        shards,
        mesh=mesh,
        in_specs=(placed, placed, placed, P("dp", None), placed, P(None, "tensor"), P("tensor"), placed, placed),
        out_specs=(placed,) * 6 + (P("tensor"),),
        check_vma=False,
    )
```

```python
import functools

import jax
import jax.numpy as jnp
from jax import lax
from jax.experimental import pallas as pl
from jax.experimental.pallas import tpu as pltpu
from jax.sharding import PartitionSpec as P

MESH = pl.DeviceIdType.MESH
F32 = jnp.float32
BF16 = jnp.bfloat16

D = 5120
HEAD_DIM = 128
LEN = 384
WIDTH = 640
HEADS = WIDTH // HEAD_DIM
CA = 256
CB = WIDTH - CA
HALF = LEN // 2
QUARTER = HALF // 2
OUT_ROWS = 160
HALF_ROWS = OUT_ROWS // 2
SCALE = HEAD_DIM ** (-0.5)
EPSILON = 1e-05
MESSAGES = 128
VMEM_LIMIT = 51 << 20


def dot(a, b, ca, cb):
    return lax.dot_general(a, b, (((ca,), (cb,)), ((), ())), preferred_element_type=F32)


def kernel(
    q_hbm, k_hbm, v_hbm, mask_hbm, res_hbm, w_hbm, gain_hbm, ups_hbm, rg_hbm,
    lo, gr, gq, gk, gv, gw_out, gg_ref,
    q, k, v, mask_ref, res, w, gain_ref, ups, rg, bias, probs, att, ga, gacc,
    pa, pb, rec_az, rec_a, rec_b, mer_a, mer_b, zb_send, zb_rec, own,
    stat, stat_rec, all_a, all_b,
    gwb, cx_rec, u, x_rec, x_mer, z_send, z_rec, z_mer, z_own,
    gain0, gain0_rec, gain1, gain1_rec, gain2, gain2_rec,
    ssem, rsem, lsem,
):
    t = lax.axis_index("tensor")
    dp = lax.axis_index("dp")
    z, y = t // 4, t % 4
    c, x, zh = dp % 2, (dp // 2) % 4, dp // 8

    def at_y(step):
        return {"tensor": z * 4 + (y + step) % 4}

    z_peer = {"tensor": (1 - z) * 4 + y}
    c_peer = {"dp": dp + 1 - 2 * c}

    def at_x(step):
        return {"dp": zh * 8 + ((x + step) % 4) * 2 + c}

    def at_zh(step):
        return {"dp": ((zh + step) % 4) * 8 + x * 2 + c}

    peers = [{"tensor": (t + j) % 8} for j in range(1, 8)]
    peers += [c_peer]
    peers += [at_x(s) for s in (1, 2, 3)]
    peers += [at_zh(s) for s in (1, 2, 3)]

    local = []

    def fetch(src, dst):
        copy = pltpu.make_async_copy(src, dst, lsem.at[len(local)])
        local.append(copy)
        copy.start()
        return copy

    in_mask = fetch(mask_hbm, mask_ref)
    in_q, in_k, in_v = fetch(q_hbm, q), fetch(k_hbm, k), fetch(v_hbm, v)
    in_w = fetch(w_hbm, w)
    in_gain = fetch(gain_hbm, gain_ref)
    in_res, in_ups, in_rg = fetch(res_hbm, res), fetch(ups_hbm, ups), fetch(rg_hbm, rg)

    barrier = pltpu.get_barrier_semaphore()
    for peer in peers:
        pl.semaphore_signal(barrier, inc=1, device_id=peer, device_id_type=MESH)

    messages = []

    def message(src, dst, device, start=True):
        i = len(messages)
        copy = pltpu.make_async_remote_copy(
            src_ref=src, dst_ref=dst, send_sem=ssem.at[i], recv_sem=rsem.at[i],
            device_id=device, device_id_type=MESH,
        )
        messages.append(copy)
        if start:
            copy.start()
        return copy

    in_mask.wait()
    zeros = jnp.sum(1 - mask_ref[...], axis=1, keepdims=True)
    row = lax.broadcasted_iota(jnp.int32, (LEN, LEN), 0)
    col = lax.broadcasted_iota(jnp.int32, (LEN, LEN), 1)
    allowed = (col <= row) | (jnp.maximum(row, col) < zeros)
    bias[...] = jnp.where(allowed, 0.0, -jnp.inf).astype(F32)
    in_q.wait()
    in_k.wait()
    in_v.wait()

    def head_cols(h):
        return pl.ds(pl.multiple_of(h * HEAD_DIM, HEAD_DIM), HEAD_DIM)

    units = (pl.ds(0, HALF), pl.ds(HALF, HALF))
    firsts = (pl.ds(0, QUARTER), pl.ds(HALF, QUARTER))
    seconds = (pl.ds(QUARTER, QUARTER), pl.ds(HALF + QUARTER, QUARTER))

    def attend(n):
        rows = units[n]

        def forward(h, carry):
            cols = head_cols(h)
            s = dot(q[rows, cols], k[:, cols], 1, 1) * SCALE + bias[rows]
            e = jnp.exp(s - jnp.max(s, axis=1, keepdims=True))
            p = e * (1.0 / jnp.sum(e, axis=1, keepdims=True))
            probs[h, rows] = p
            att[rows, cols] = dot(p.astype(BF16), v[:, cols], 1, 0).astype(BF16)
            return carry

        lax.fori_loop(0, HEADS, forward, 0, unroll=True)

    def w_rows(block):
        return pl.ds(pl.multiple_of(block * WIDTH, WIDTH), WIDTH)

    def project(n, d):
        rows = units[n]

        def one(j, carry):
            zz = j * z + (1 - j) * (1 - z)
            block = zz * 4 + (y + d) % 4
            r = dot(att[rows], w[w_rows(block), :], 1, 1)
            pa[d, j, rows] = r[:, :CA].astype(BF16)
            pb[d, zz, rows] = r[:, CA:].astype(BF16)
            return carry

        lax.fori_loop(0, 2, one, 0)

    rs = {}

    def send_far(n):
        rs["b", n, 0] = message(pb.at[2, :, firsts[n]], rec_b.at[n, 0], at_y(1))
        rs["b", n, 1] = message(pb.at[2, :, seconds[n]], rec_b.at[n, 1], at_y(-1))

    def send_up(n):
        rs["b", n, 2] = message(pb.at[1, :, seconds[n]], rec_b.at[n, 2], at_y(1))

    def send_down(n):
        rs["b", n, 3] = message(pb.at[3, :, firsts[n]], rec_b.at[n, 3], at_y(-1))

    def send_z(n, d):
        rs["z", n, d] = message(pa.at[d, 0, units[n]], rec_az.at[d, units[n]], z_peer)

    def merge_b(n):
        rs["b", n, 0].wait_recv()
        mer_b[n, 0] = pb[1, :, firsts[n]] + rec_b[n, 0]
        rs["b", n, 4] = message(mer_b.at[n, 0], rec_b.at[n, 4], at_y(1))
        rs["b", n, 1].wait_recv()
        mer_b[n, 1] = pb[3, :, seconds[n]] + rec_b[n, 1]
        rs["b", n, 5] = message(mer_b.at[n, 1], rec_b.at[n, 5], at_y(-1))

    def join(n, d):
        rs["z", n, d].wait_recv()
        pa[d, 1, units[n]] = pa[d, 1, units[n]] + rec_az[d, units[n]]

    def join_far(n):
        join(n, 2)
        rs["a", n, 0] = message(pa.at[2, 1, firsts[n]], rec_a.at[n, 0], at_y(1))
        rs["a", n, 1] = message(pa.at[2, 1, seconds[n]], rec_a.at[n, 1], at_y(-1))

    def join_up(n):
        join(n, 1)
        rs["a", n, 2] = message(pa.at[1, 1, seconds[n]], rec_a.at[n, 2], at_y(1))

    def join_down(n):
        join(n, 3)
        rs["a", n, 3] = message(pa.at[3, 1, firsts[n]], rec_a.at[n, 3], at_y(-1))

    def merge_a(n):
        rs["a", n, 0].wait_recv()
        mer_a[n, 0] = pa[1, 1, firsts[n]] + rec_a[n, 0]
        rs["a", n, 4] = message(mer_a.at[n, 0], rec_a.at[n, 4], at_y(1))
        rs["a", n, 1].wait_recv()
        mer_a[n, 1] = pa[3, 1, seconds[n]] + rec_a[n, 1]
        rs["a", n, 5] = message(mer_a.at[n, 1], rec_a.at[n, 5], at_y(-1))

    def b_sum(n, zz):
        top = pb[0, zz, firsts[n]].astype(F32) + rec_b[n, 3, zz].astype(F32) + rec_b[n, 4, zz].astype(F32)
        low = pb[0, zz, seconds[n]].astype(F32) + rec_b[n, 2, zz].astype(F32) + rec_b[n, 5, zz].astype(F32)
        return top, low

    def cross_b(n):
        for i in (2, 3, 4, 5):
            rs["b", n, i].wait_recv()
        top, low = b_sum(n, 1 - z)
        zb_send[firsts[n]] = top.astype(BF16)
        zb_send[seconds[n]] = low.astype(BF16)
        rs["zb", n] = message(zb_send.at[units[n]], zb_rec.at[units[n]], z_peer)
        top, low = b_sum(n, z)
        own[firsts[n], CA:] = top
        own[seconds[n], CA:] = low

    def finish(n):
        rows = units[n]
        rs["z", n, 0].wait_recv()
        for i in (2, 3, 4, 5):
            rs["a", n, i].wait_recv()
        add_top = rec_a[n, 3].astype(F32) + rec_a[n, 4].astype(F32)
        add_low = rec_a[n, 2].astype(F32) + rec_a[n, 5].astype(F32)
        for part, add in ((firsts[n], add_top), (seconds[n], add_low)):
            total = pa[0, 1, part].astype(F32) + rec_az[0, part].astype(F32) + add
            lo[part, :CA] = (total + res[part, :CA].astype(F32)).astype(BF16)
        f_a = lo[rows, :CA].astype(F32)
        scaled_a = ups[rows, :CA].astype(F32) * gain_row[:, :CA]
        square = jnp.sum(f_a * f_a, axis=1, keepdims=True)
        inner = jnp.sum(f_a * scaled_a, axis=1, keepdims=True)
        rs["zb", n].wait_recv()
        own_b = own[rows, CA:] + zb_rec[rows].astype(F32) + res[rows, CA:].astype(F32)
        low_b = own_b.astype(BF16)
        lo[rows, CA:] = low_b
        f_b = low_b.astype(F32)
        scaled_b = ups[rows, CA:].astype(F32) * gain_row[:, CA:]
        square = square + jnp.sum(f_b * f_b, axis=1, keepdims=True)
        inner = inner + jnp.sum(f_b * scaled_b, axis=1, keepdims=True)
        lane = lax.broadcasted_iota(jnp.int32, (HALF, 128), 1)
        packed = jnp.where(lane == 0, square, jnp.where(lane == 1, inner, 0.0))
        packed = jnp.concatenate([packed, jnp.zeros((64, 128), F32)], axis=0)
        stat[n] = packed.T[:8]
        for j in range(1, 8):
            rs["s", n, j] = message(stat.at[n], stat_rec.at[n, j], peers[j - 1])

    ag = {}

    def gradient(n):
        rows = units[n]
        total = stat[n]
        for j in range(1, 8):
            rs["s", n, j].wait_recv()
            total = total + stat_rec[n, j]
        wide = jnp.concatenate([total, jnp.zeros((120, 256), F32)], axis=0).T[:HALF]
        square, inner = wide[:, 0:1], wide[:, 1:2]
        rms = jnp.sqrt(square / D + EPSILON)
        back = 1.0 / rms
        row_inner = inner / (rms * D)
        cut = (slice(0, CA), slice(CA, WIDTH))
        for buf, cols in zip((all_a, all_b), cut):
            up = ups[rows, cols].astype(F32)
            normed = lo[rows, cols].astype(F32) * back
            g = rg[rows, cols].astype(F32) + (up * gain_row[:, cols] - normed * row_inner) * back
            g = g.astype(BF16)
            buf[t, rows] = g
            gr[rows, cols] = g
            share = (up * normed).reshape(HALF // 8, 8, -1).sum(axis=0)
            if n == 0:
                gain0[:, cols] = share
            else:
                gain0[:, cols] += share
        ag["zb", n] = message(all_b.at[t, rows], all_b.at[t, rows], z_peer)
        for key, buf in (("a", all_a), ("b", all_b)):
            send_half(key, buf, t, n, 1, firsts[n], 1)
            send_half(key, buf, t, n, -1, seconds[n], 1)

    def send_rest(n):
        rows = units[n]
        ag["za", n, 0] = message(all_a.at[t, rows], all_a.at[t, rows], z_peer)
        for key, buf in (("a", all_a), ("b", all_b)):
            send_half(key, buf, t, n, 1, seconds[n], 2)
            send_half(key, buf, t, n, -1, firsts[n], 2)

    def send_half(key, buf, block, n, step, rows, turn):
        part = buf.at[block, rows]
        ag[key, n, step, turn] = message(part, part, at_y(step))

    def block_at(zz, step):
        return zz * 4 + (y + step) % 4

    def forward_on(key, buf, zz, n):
        ag[key, n, 1, 1].wait_recv()
        send_half(key, buf, block_at(zz, -1), n, 1, firsts[n], 3)
        ag[key, n, -1, 1].wait_recv()
        send_half(key, buf, block_at(zz, 1), n, -1, seconds[n], 3)

    def arrived(key, n, turn):
        ag[key, n, 1, turn].wait_recv()
        ag[key, n, -1, turn].wait_recv()

    def partner(n):
        ag["zb", n].wait_recv()
        block = block_at(1 - z, 0)
        send_half("p", all_b, block, n, 1, firsts[n], 1)
        send_half("p", all_b, block, n, -1, seconds[n], 1)
        send_half("p", all_b, block, n, 1, seconds[n], 2)
        send_half("p", all_b, block, n, -1, firsts[n], 2)

    def across(step, n):
        part = all_a.at[block_at(z, step), units[n]]
        ag["za", n, step] = message(part, part, z_peer)

    def accumulate(blocks, start):
        def one(j, carry):
            block = blocks(j)
            grad = jnp.concatenate([all_a[block], all_b[block]], axis=1)
            r = dot(grad, w[w_rows(block), :], 1, 0)
            if start:
                gacc[...] = r
            else:
                gacc[...] += r
            return carry

        lax.fori_loop(0, 1 if start else 2, one, 0)

    attend(0)
    in_w.wait()
    project(0, 2)
    pl.semaphore_wait(barrier, len(peers))
    send_far(0)
    send_z(0, 2)
    project(0, 1)
    send_up(0)
    send_z(0, 1)
    project(0, 3)
    send_down(0)
    send_z(0, 3)
    project(0, 0)
    send_z(0, 0)
    attend(1)
    project(1, 2)
    merge_b(0)
    send_far(1)
    send_z(1, 2)
    join_far(0)
    project(1, 1)
    send_up(1)
    send_z(1, 1)
    project(1, 3)
    send_down(1)
    join_up(0)
    join_down(0)
    project(1, 0)
    in_res.wait()
    in_ups.wait()
    in_gain.wait()
    in_rg.wait()
    gain_row = gain_ref[...].reshape(1, WIDTH)
    cross_b(0)
    send_z(1, 3)
    send_z(1, 0)
    merge_a(0)
    merge_b(1)
    join_far(1)
    join_up(1)
    finish(0)
    join_down(1)
    cross_b(1)
    merge_a(1)
    gradient(0)
    finish(1)
    send_rest(0)
    forward_on("a", all_a, z, 0)
    forward_on("b", all_b, z, 0)
    gradient(1)
    send_rest(1)
    gain_c = message(gain0, gain0_rec, c_peer)

    order = [t, block_at(1 - z, 0), block_at(z, -1), block_at(z, 1), block_at(z, 2)]
    order += [block_at(1 - z, -1), block_at(1 - z, 1), block_at(1 - z, 2)]
    cx = {}

    def weight_grad(i):
        grad = jnp.concatenate([all_a[order[i]], all_b[order[i]]], axis=1)
        r = dot(grad, att[...], 0, 0).astype(BF16)
        for s in range(4):
            gwb[i, s % 2, s // 2] = r[s * OUT_ROWS : (s + 1) * OUT_ROWS]
        cx[i] = message(gwb.at[i, 1 - c], cx_rec.at[i], c_peer)

    low_rows, high_rows = pl.ds(0, HALF_ROWS), pl.ds(HALF_ROWS, HALF_ROWS)
    waits = []

    def has(i, d):
        return (x + d) % 4 // 2 == order[i] % 2

    def start_when(condition, *made):
        waits.extend((condition, make) for make in made)
        for make in made:
            make().start()

    X_SEM, Z_SEM = MESSAGES, MESSAGES + 48

    def x_copy(i, kind, src, step):
        sem = X_SEM + 6 * i + kind
        return pltpu.make_async_remote_copy(
            src_ref=src, dst_ref=x_rec.at[i, kind], send_sem=ssem.at[sem], recv_sem=rsem.at[sem],
            device_id=at_x(step), device_id_type=MESH,
        )

    def x_far(i, src, step):
        sem = X_SEM + 6 * i
        return pltpu.make_async_remote_copy(
            src_ref=src, dst_ref=x_rec.at[i, 0], send_sem=ssem.at[sem + (5 if step < 0 else 0)],
            recv_sem=rsem.at[sem], device_id=at_x(step), device_id_type=MESH,
        )

    def z_copy(kind, src, step):
        sem = Z_SEM + kind
        return pltpu.make_async_remote_copy(
            src_ref=src, dst_ref=z_rec.at[kind], send_sem=ssem.at[sem], recv_sem=rsem.at[sem],
            device_id=at_zh(step), device_id_type=MESH,
        )

    def x_first(i):
        cx[i].wait_recv()
        u[i] = gwb[i, c] + cx_rec[i]
        far, near, back_near = (x + 2) % 2, (x + 1) % 2, (x + 3) % 2
        is_far, is_next, is_back = has(i, 2), has(i, 1), has(i, 3)

        @pl.when(is_far)
        def _():
            start_when(
                is_far,
                lambda: x_far(i, u.at[i, far, low_rows], 1),
                lambda: x_far(i, u.at[i, far, high_rows], -1),
            )

        @pl.when(is_next)
        def _():
            start_when(is_next, lambda: x_copy(i, 1, u.at[i, near, high_rows], 1))

        @pl.when(is_back)
        def _():
            start_when(is_back, lambda: x_copy(i, 3, u.at[i, back_near, low_rows], -1))

    def x_second(i):
        near, back_near = (x + 1) % 2, (x + 3) % 2
        is_next, is_back = has(i, 1), has(i, 3)

        @pl.when(is_next)
        def _():
            x_far(i, x_mer.at[i], 1).wait_recv()
            x_mer[i] = u[i, near, :HALF_ROWS] + x_rec[i, 0]
            start_when(is_next, lambda: x_copy(i, 2, x_mer.at[i], 1))

        @pl.when(is_back)
        def _():
            x_far(i, x_mer.at[i], -1).wait_recv()
            x_mer[i] = u[i, back_near, HALF_ROWS:] + x_rec[i, 0]
            start_when(is_back, lambda: x_copy(i, 4, x_mer.at[i], -1))

    def x_last(i):
        kk = order[i] // 2
        e = (kk - zh) % 4
        mine = has(i, 0)
        is_far, is_next, is_back = mine & (e == 2), mine & (e == 1), mine & (e == 3)

        @pl.when(mine)
        def _():
            for kind in (1, 2, 3, 4):
                x_copy(i, kind, x_mer.at[i], 1).wait_recv()
            upper = u[i, x % 2, :HALF_ROWS].astype(F32) + x_rec[i, 2].astype(F32) + x_rec[i, 3].astype(F32)
            lower = u[i, x % 2, HALF_ROWS:].astype(F32) + x_rec[i, 1].astype(F32) + x_rec[i, 4].astype(F32)
            z_send[i, :HALF_ROWS] = upper.astype(BF16)
            z_send[i, HALF_ROWS:] = lower.astype(BF16)

            @pl.when(e == 0)
            def _():
                z_own[:HALF_ROWS] = upper
                z_own[HALF_ROWS:] = lower

        @pl.when(is_far)
        def _():
            start_when(
                is_far,
                lambda: z_copy(0, z_send.at[i, low_rows], 1),
                lambda: z_copy(1, z_send.at[i, high_rows], -1),
            )

        @pl.when(is_next)
        def _():
            start_when(is_next, lambda: z_copy(2, z_send.at[i, high_rows], 1))

        @pl.when(is_back)
        def _():
            start_when(is_back, lambda: z_copy(4, z_send.at[i, low_rows], -1))

    def z_second(i):
        e = (order[i] // 2 - zh) % 4
        is_next, is_back = has(i, 0) & (e == 1), has(i, 0) & (e == 3)

        @pl.when(is_next)
        def _():
            z_copy(0, z_mer.at[0], 1).wait_recv()
            z_mer[0] = z_send[i, :HALF_ROWS] + z_rec[0]
            start_when(is_next, lambda: z_copy(3, z_mer.at[0], 1))

        @pl.when(is_back)
        def _():
            z_copy(1, z_mer.at[1], -1).wait_recv()
            z_mer[1] = z_send[i, HALF_ROWS:] + z_rec[1]
            start_when(is_back, lambda: z_copy(5, z_mer.at[1], -1))

    weight_grad(0)
    arrived("a", 0, 2)
    across(-1, 0)
    across(1, 0)
    partner(0)
    forward_on("a", all_a, z, 1)
    arrived("a", 0, 3)
    across(2, 0)
    forward_on("b", all_b, z, 1)
    partner(1)
    x_first(0)
    arrived("a", 1, 2)
    across(-1, 1)
    across(1, 1)
    arrived("b", 0, 2)
    arrived("b", 1, 2)
    weight_grad(2)
    weight_grad(3)
    forward_on("p", all_b, 1 - z, 0)
    x_first(2)
    x_first(3)
    ag["za", 0, 0].wait_recv()
    ag["za", 1, 0].wait_recv()
    weight_grad(1)
    gain_c.wait_recv()
    gain1[...] = gain0[...] + gain0_rec[...]
    gain_x = [message(gain1, gain1_rec.at[s - 1], at_x(s)) for s in (1, 2, 3)]
    x_second(0)
    accumulate(lambda j: t, True)
    x_first(1)
    arrived("a", 1, 3)
    across(2, 1)
    arrived("b", 0, 3)
    arrived("b", 1, 3)
    weight_grad(4)
    forward_on("p", all_b, 1 - z, 1)
    accumulate(lambda j: order[3] * j + order[2] * (1 - j), False)
    x_second(2)
    x_first(4)
    x_second(3)
    for n in (0, 1):
        ag["za", n, -1].wait_recv()
        ag["za", n, 1].wait_recv()
        arrived("p", n, 2)
    weight_grad(5)
    weight_grad(6)
    x_second(1)
    x_last(0)
    x_first(5)
    x_first(6)
    accumulate(lambda j: order[4] * j + order[1] * (1 - j), False)
    for n in (0, 1):
        ag["za", n, 2].wait_recv()
        arrived("p", n, 3)
    weight_grad(7)
    x_second(4)
    x_last(2)
    x_first(7)
    for copy in gain_x:
        copy.wait_recv()
    gain2[...] = gain1[...] + gain1_rec[0] + gain1_rec[1] + gain1_rec[2]
    gain_z = [message(gain2, gain2_rec.at[s - 1], at_zh(s)) for s in (1, 2, 3)]
    x_last(1)
    accumulate(lambda j: order[6] * j + order[5] * (1 - j), False)
    x_last(3)
    x_second(5)
    last = order[7]
    grad = jnp.concatenate([all_a[last], all_b[last]], axis=1)
    ga[...] = (gacc[...] + dot(grad, w[w_rows(last), :], 1, 0)).astype(BF16)
    x_last(4)
    x_second(6)
    z_second(0)
    x_second(7)

    def backward(h, carry):
        cols = head_cols(h)
        g_head = ga[:, cols]
        p = probs[h]
        gv[:, cols] = dot(p.astype(BF16), g_head, 0, 0).astype(BF16)
        gp = dot(g_head, v[:, cols], 1, 1)
        delta = jnp.sum(p * gp, axis=1, keepdims=True)
        gs = (p * (gp - delta) * SCALE).astype(BF16)
        gq[:, cols] = dot(gs, k[:, cols], 1, 0).astype(BF16)
        gk[:, cols] = dot(gs, q[:, cols], 0, 0).astype(BF16)
        return carry

    lax.fori_loop(0, 2, backward, 0)
    z_second(2)
    z_second(1)
    x_last(5)
    lax.fori_loop(2, 3, backward, 0)
    x_last(6)
    x_last(7)
    lax.fori_loop(3, HEADS, backward, 0)
    for copy in gain_z:
        copy.wait_recv()
    gain = gain2[...] + gain2_rec[0] + gain2_rec[1] + gain2_rec[2]
    gg_ref[...] = jnp.sum(gain, axis=0)
    z_second(3)
    z_second(4)
    z_second(5)
    z_second(6)
    z_second(7)

    for kind in (2, 3, 4, 5):
        z_copy(kind, z_mer.at[0], 1).wait_recv()
    gw_out[:HALF_ROWS] = z_own[:HALF_ROWS] + z_rec[3].astype(F32) + z_rec[4].astype(F32)
    gw_out[HALF_ROWS:] = z_own[HALF_ROWS:] + z_rec[2].astype(F32) + z_rec[5].astype(F32)

    for copy in messages:
        copy.wait_send()
    for condition, make in waits:

        @pl.when(condition)
        def _():
            make().wait_send()

    assert len(messages) <= MESSAGES


def hand_over(*refs):
    n = len(refs) // 2
    sources, outs, sems = refs[:n], refs[n : 2 * n], refs[2 * n]
    copies = [pltpu.make_async_copy(a, b, sems.at[i]) for i, (a, b) in enumerate(zip(sources, outs))]
    for copy in copies:
        copy.start()
    for copy in copies:
        copy.wait()


def deliver(arrays):
    vmem = pl.BlockSpec(memory_space=pltpu.VMEM)
    return pl.pallas_call(
        hand_over,
        out_shape=[jax.ShapeDtypeStruct(a.shape, a.dtype) for a in arrays],
        in_specs=[vmem] * len(arrays),
        out_specs=[pl.BlockSpec(memory_space=pl.ANY)] * len(arrays),
        scratch_shapes=[pltpu.SemaphoreType.DMA((len(arrays),))],
        compiler_params=pltpu.CompilerParams(vmem_limit_bytes=8 << 20),
    )(*arrays)


def shards(q, k, v, mask, res, w, gain, ups, rg):
    rows = jax.ShapeDtypeStruct((LEN, WIDTH), BF16)
    hbm = pl.BlockSpec(memory_space=pltpu.HBM)
    vmem = pl.BlockSpec(memory_space=pltpu.VMEM)

    def b(*shape):
        return pltpu.VMEM(shape, BF16)

    def f(*shape):
        return pltpu.VMEM(shape, F32)

    slab = (LEN, WIDTH)
    part = (OUT_ROWS, WIDTH)
    half = (HALF_ROWS, WIDTH)
    scratch = [
        b(*slab), b(*slab), b(*slab), pltpu.VMEM((1, LEN), jnp.int32), b(*slab), b(D, WIDTH), f(WIDTH), b(*slab), b(*slab),
        f(LEN, LEN), f(HEADS, LEN, LEN), b(*slab), b(*slab), f(*slab),
        b(4, 2, LEN, CA), b(4, 2, LEN, CB), b(4, LEN, CA), b(2, 6, QUARTER, CA), b(2, 6, 2, QUARTER, CB),
        b(2, 2, QUARTER, CA), b(2, 2, 2, QUARTER, CB), b(LEN, CB), b(LEN, CB), f(*slab),
        f(2, 8, 256), f(2, 8, 8, 256), b(8, LEN, CA), b(8, LEN, CB),
        b(8, 2, 2, *part), b(8, 2, *part), b(8, 2, *part), b(8, 5, *half), b(8, *half),
        b(8, *part), b(6, *half), b(2, *half), f(*part),
        f(8, WIDTH), f(8, WIDTH), f(8, WIDTH), f(3, 8, WIDTH), f(8, WIDTH), f(3, 8, WIDTH),
        pltpu.SemaphoreType.DMA((MESSAGES + 54,)),
        pltpu.SemaphoreType.DMA((MESSAGES + 54,)),
        pltpu.SemaphoreType.DMA((16,)),
    ]
    outs = pl.pallas_call(
        kernel,
        out_shape=(
            rows, rows, rows, rows, rows,
            jax.ShapeDtypeStruct(part, F32),
            jax.ShapeDtypeStruct((WIDTH,), F32),
        ),
        in_specs=[hbm] * 9,
        out_specs=(vmem,) * 7,
        scratch_shapes=scratch,
        compiler_params=pltpu.CompilerParams(
            collective_id=0, has_side_effects=True, vmem_limit_bytes=VMEM_LIMIT
        ),
    )(q, k, v, mask, res, w, gain, ups, rg)
    return deliver(outs)


def solution(mesh):
    placed = P("dp", "tensor")
    return jax.shard_map(
        shards,
        mesh=mesh,
        in_specs=(placed, placed, placed, P("dp", None), placed, P(None, "tensor"), P("tensor"), placed, placed),
        out_specs=(placed,) * 6 + (P("tensor"),),
        check_vma=False,
    )
```

```python
import functools

import jax
import jax.numpy as jnp
from jax import lax
from jax.experimental import pallas as pl
from jax.experimental.pallas import tpu as pltpu
from jax.sharding import PartitionSpec as P

MESH = pl.DeviceIdType.MESH
F32 = jnp.float32
BF16 = jnp.bfloat16

D = 5120
HEAD_DIM = 128
LEN = 384
WIDTH = 640
HEADS = WIDTH // HEAD_DIM
CA = 256
CB = WIDTH - CA
HALF = LEN // 2
QUARTER = HALF // 2
OUT_ROWS = 160
HALF_ROWS = OUT_ROWS // 2
SCALE = HEAD_DIM ** (-0.5)
EPSILON = 1e-05
MESSAGES = 128
VMEM_LIMIT = 51 << 20


def dot(a, b, ca, cb):
    return lax.dot_general(a, b, (((ca,), (cb,)), ((), ())), preferred_element_type=F32)


def kernel(
    q_hbm, k_hbm, v_hbm, mask_hbm, res_hbm, w_hbm, gain_hbm, ups_hbm, rg_hbm,
    lo, gr, gq, gk, gv, gw_out, gg_ref,
    q, k, v, mask_ref, res, w, gain_ref, ups, rg, bias, probs, att, ga, gacc,
    pa, pb, rec_az, rec_a, rec_b, mer_a, mer_b, zb_send, zb_rec, own,
    stat, stat_rec, all_a, all_b,
    gwb, cx_rec, u, x_rec, x_mer, z_send, z_rec, z_mer, z_own,
    gain0, gain0_rec, gain1, gain1_rec, gain2, gain2_rec,
    ssem, rsem, lsem,
):
    t = lax.axis_index("tensor")
    dp = lax.axis_index("dp")
    z, y = t // 4, t % 4
    c, x, zh = dp % 2, (dp // 2) % 4, dp // 8

    def at_y(step):
        return {"tensor": z * 4 + (y + step) % 4}

    z_peer = {"tensor": (1 - z) * 4 + y}
    c_peer = {"dp": dp + 1 - 2 * c}

    def at_x(step):
        return {"dp": zh * 8 + ((x + step) % 4) * 2 + c}

    def at_zh(step):
        return {"dp": ((zh + step) % 4) * 8 + x * 2 + c}

    peers = [{"tensor": (t + j) % 8} for j in range(1, 8)]
    peers += [c_peer]
    peers += [at_x(s) for s in (1, 2, 3)]
    peers += [at_zh(s) for s in (1, 2, 3)]

    local = []

    def fetch(src, dst):
        copy = pltpu.make_async_copy(src, dst, lsem.at[len(local)])
        local.append(copy)
        copy.start()
        return copy

    in_mask = fetch(mask_hbm, mask_ref)
    in_q, in_k, in_v = fetch(q_hbm, q), fetch(k_hbm, k), fetch(v_hbm, v)
    in_w = fetch(w_hbm, w)
    in_gain = fetch(gain_hbm, gain_ref)
    in_res, in_ups, in_rg = fetch(res_hbm, res), fetch(ups_hbm, ups), fetch(rg_hbm, rg)

    barrier = pltpu.get_barrier_semaphore()
    for peer in peers:
        pl.semaphore_signal(barrier, inc=1, device_id=peer, device_id_type=MESH)

    messages = []

    def message(src, dst, device, start=True):
        i = len(messages)
        copy = pltpu.make_async_remote_copy(
            src_ref=src, dst_ref=dst, send_sem=ssem.at[i], recv_sem=rsem.at[i],
            device_id=device, device_id_type=MESH,
        )
        messages.append(copy)
        if start:
            copy.start()
        return copy

    in_mask.wait()
    zeros = jnp.sum(1 - mask_ref[...], axis=1, keepdims=True)
    row = lax.broadcasted_iota(jnp.int32, (LEN, LEN), 0)
    col = lax.broadcasted_iota(jnp.int32, (LEN, LEN), 1)
    allowed = (col <= row) | (jnp.maximum(row, col) < zeros)
    bias[...] = jnp.where(allowed, 0.0, -jnp.inf).astype(F32)
    in_q.wait()
    in_k.wait()
    in_v.wait()

    def head_cols(h):
        return pl.ds(pl.multiple_of(h * HEAD_DIM, HEAD_DIM), HEAD_DIM)

    units = (pl.ds(0, HALF), pl.ds(HALF, HALF))
    firsts = (pl.ds(0, QUARTER), pl.ds(HALF, QUARTER))
    seconds = (pl.ds(QUARTER, QUARTER), pl.ds(HALF + QUARTER, QUARTER))

    def attend(n):
        rows = units[n]

        def forward(h, carry):
            cols = head_cols(h)
            s = dot(q[rows, cols], k[:, cols], 1, 1) * SCALE + bias[rows]
            e = jnp.exp(s - jnp.max(s, axis=1, keepdims=True))
            p = e * (1.0 / jnp.sum(e, axis=1, keepdims=True))
            probs[h, rows] = p
            att[rows, cols] = dot(p.astype(BF16), v[:, cols], 1, 0).astype(BF16)
            return carry

        lax.fori_loop(0, HEADS, forward, 0, unroll=True)

    def w_rows(block):
        return pl.ds(pl.multiple_of(block * WIDTH, WIDTH), WIDTH)

    def project(n, d):
        rows = units[n]

        def one(j, carry):
            zz = j * z + (1 - j) * (1 - z)
            block = zz * 4 + (y + d) % 4
            r = dot(att[rows], w[w_rows(block), :], 1, 1)
            pa[d, j, rows] = r[:, :CA].astype(BF16)
            pb[d, zz, rows] = r[:, CA:].astype(BF16)
            return carry

        lax.fori_loop(0, 2, one, 0)

    rs = {}

    def send_far(n):
        rs["b", n, 0] = message(pb.at[2, :, firsts[n]], rec_b.at[n, 0], at_y(1))
        rs["b", n, 1] = message(pb.at[2, :, seconds[n]], rec_b.at[n, 1], at_y(-1))

    def send_up(n):
        rs["b", n, 2] = message(pb.at[1, :, seconds[n]], rec_b.at[n, 2], at_y(1))

    def send_down(n):
        rs["b", n, 3] = message(pb.at[3, :, firsts[n]], rec_b.at[n, 3], at_y(-1))

    def send_z(n, d):
        rs["z", n, d] = message(pa.at[d, 0, units[n]], rec_az.at[d, units[n]], z_peer)

    def merge_b(n):
        rs["b", n, 0].wait_recv()
        mer_b[n, 0] = pb[1, :, firsts[n]] + rec_b[n, 0]
        rs["b", n, 4] = message(mer_b.at[n, 0], rec_b.at[n, 4], at_y(1))
        rs["b", n, 1].wait_recv()
        mer_b[n, 1] = pb[3, :, seconds[n]] + rec_b[n, 1]
        rs["b", n, 5] = message(mer_b.at[n, 1], rec_b.at[n, 5], at_y(-1))

    def join(n, d):
        rs["z", n, d].wait_recv()
        pa[d, 1, units[n]] = pa[d, 1, units[n]] + rec_az[d, units[n]]

    def join_far(n):
        join(n, 2)
        rs["a", n, 0] = message(pa.at[2, 1, firsts[n]], rec_a.at[n, 0], at_y(1))
        rs["a", n, 1] = message(pa.at[2, 1, seconds[n]], rec_a.at[n, 1], at_y(-1))

    def join_up(n):
        join(n, 1)
        rs["a", n, 2] = message(pa.at[1, 1, seconds[n]], rec_a.at[n, 2], at_y(1))

    def join_down(n):
        join(n, 3)
        rs["a", n, 3] = message(pa.at[3, 1, firsts[n]], rec_a.at[n, 3], at_y(-1))

    def merge_a(n):
        rs["a", n, 0].wait_recv()
        mer_a[n, 0] = pa[1, 1, firsts[n]] + rec_a[n, 0]
        rs["a", n, 4] = message(mer_a.at[n, 0], rec_a.at[n, 4], at_y(1))
        rs["a", n, 1].wait_recv()
        mer_a[n, 1] = pa[3, 1, seconds[n]] + rec_a[n, 1]
        rs["a", n, 5] = message(mer_a.at[n, 1], rec_a.at[n, 5], at_y(-1))

    def b_sum(n, zz):
        top = pb[0, zz, firsts[n]].astype(F32) + rec_b[n, 3, zz].astype(F32) + rec_b[n, 4, zz].astype(F32)
        low = pb[0, zz, seconds[n]].astype(F32) + rec_b[n, 2, zz].astype(F32) + rec_b[n, 5, zz].astype(F32)
        return top, low

    def cross_b(n):
        for i in (2, 3, 4, 5):
            rs["b", n, i].wait_recv()
        top, low = b_sum(n, 1 - z)
        zb_send[firsts[n]] = top.astype(BF16)
        zb_send[seconds[n]] = low.astype(BF16)
        rs["zb", n] = message(zb_send.at[units[n]], zb_rec.at[units[n]], z_peer)
        top, low = b_sum(n, z)
        own[firsts[n], CA:] = top
        own[seconds[n], CA:] = low

    def finish(n):
        rows = units[n]
        rs["z", n, 0].wait_recv()
        for i in (2, 3, 4, 5):
            rs["a", n, i].wait_recv()
        add_top = rec_a[n, 3].astype(F32) + rec_a[n, 4].astype(F32)
        add_low = rec_a[n, 2].astype(F32) + rec_a[n, 5].astype(F32)
        for part, add in ((firsts[n], add_top), (seconds[n], add_low)):
            total = pa[0, 1, part].astype(F32) + rec_az[0, part].astype(F32) + add
            lo[part, :CA] = (total + res[part, :CA].astype(F32)).astype(BF16)
        f_a = lo[rows, :CA].astype(F32)
        scaled_a = ups[rows, :CA].astype(F32) * gain_row[:, :CA]
        square = jnp.sum(f_a * f_a, axis=1, keepdims=True)
        inner = jnp.sum(f_a * scaled_a, axis=1, keepdims=True)
        rs["zb", n].wait_recv()
        own_b = own[rows, CA:] + zb_rec[rows].astype(F32) + res[rows, CA:].astype(F32)
        low_b = own_b.astype(BF16)
        lo[rows, CA:] = low_b
        f_b = low_b.astype(F32)
        scaled_b = ups[rows, CA:].astype(F32) * gain_row[:, CA:]
        square = square + jnp.sum(f_b * f_b, axis=1, keepdims=True)
        inner = inner + jnp.sum(f_b * scaled_b, axis=1, keepdims=True)
        lane = lax.broadcasted_iota(jnp.int32, (HALF, 128), 1)
        packed = jnp.where(lane == 0, square, jnp.where(lane == 1, inner, 0.0))
        packed = jnp.concatenate([packed, jnp.zeros((64, 128), F32)], axis=0)
        stat[n] = packed.T[:8]
        for j in range(1, 8):
            rs["s", n, j] = message(stat.at[n], stat_rec.at[n, j], peers[j - 1])

    ag = {}

    def gradient(n):
        rows = units[n]
        total = stat[n]
        for j in range(1, 8):
            rs["s", n, j].wait_recv()
            total = total + stat_rec[n, j]
        wide = jnp.concatenate([total, jnp.zeros((120, 256), F32)], axis=0).T[:HALF]
        square, inner = wide[:, 0:1], wide[:, 1:2]
        rms = jnp.sqrt(square / D + EPSILON)
        back = 1.0 / rms
        row_inner = inner / (rms * D)
        cut = (slice(0, CA), slice(CA, WIDTH))
        for buf, cols in zip((all_a, all_b), cut):
            up = ups[rows, cols].astype(F32)
            normed = lo[rows, cols].astype(F32) * back
            g = rg[rows, cols].astype(F32) + (up * gain_row[:, cols] - normed * row_inner) * back
            g = g.astype(BF16)
            buf[t, rows] = g
            gr[rows, cols] = g
            share = (up * normed).reshape(HALF // 8, 8, -1).sum(axis=0)
            if n == 0:
                gain0[:, cols] = share
            else:
                gain0[:, cols] += share
        ag["zb", n] = message(all_b.at[t, rows], all_b.at[t, rows], z_peer)
        for key, buf in (("a", all_a), ("b", all_b)):
            send_half(key, buf, t, n, 1, firsts[n], 1)
            send_half(key, buf, t, n, -1, seconds[n], 1)

    def send_rest(n):
        rows = units[n]
        ag["za", n, 0] = message(all_a.at[t, rows], all_a.at[t, rows], z_peer)
        for key, buf in (("a", all_a), ("b", all_b)):
            send_half(key, buf, t, n, 1, seconds[n], 2)
            send_half(key, buf, t, n, -1, firsts[n], 2)

    def send_half(key, buf, block, n, step, rows, turn):
        part = buf.at[block, rows]
        ag[key, n, step, turn] = message(part, part, at_y(step))

    def block_at(zz, step):
        return zz * 4 + (y + step) % 4

    def forward_on(key, buf, zz, n):
        ag[key, n, 1, 1].wait_recv()
        send_half(key, buf, block_at(zz, -1), n, 1, firsts[n], 3)
        ag[key, n, -1, 1].wait_recv()
        send_half(key, buf, block_at(zz, 1), n, -1, seconds[n], 3)

    def arrived(key, n, turn):
        ag[key, n, 1, turn].wait_recv()
        ag[key, n, -1, turn].wait_recv()

    def partner(n):
        ag["zb", n].wait_recv()
        block = block_at(1 - z, 0)
        send_half("p", all_b, block, n, 1, firsts[n], 1)
        send_half("p", all_b, block, n, -1, seconds[n], 1)
        send_half("p", all_b, block, n, 1, seconds[n], 2)
        send_half("p", all_b, block, n, -1, firsts[n], 2)

    def across(step, n):
        part = all_a.at[block_at(z, step), units[n]]
        ag["za", n, step] = message(part, part, z_peer)

    def accumulate(blocks, start):
        def one(j, carry):
            block = blocks(j)
            grad = jnp.concatenate([all_a[block], all_b[block]], axis=1)
            r = dot(grad, w[w_rows(block), :], 1, 0)
            if start:
                gacc[...] = r
            else:
                gacc[...] += r
            return carry

        lax.fori_loop(0, 1 if start else 2, one, 0)

    attend(0)
    in_w.wait()
    project(0, 2)
    pl.semaphore_wait(barrier, len(peers))
    send_far(0)
    send_z(0, 2)
    project(0, 1)
    send_up(0)
    send_z(0, 1)
    project(0, 3)
    send_down(0)
    send_z(0, 3)
    project(0, 0)
    send_z(0, 0)
    attend(1)
    project(1, 2)
    merge_b(0)
    send_far(1)
    send_z(1, 2)
    join_far(0)
    project(1, 1)
    send_up(1)
    send_z(1, 1)
    project(1, 3)
    send_down(1)
    join_up(0)
    join_down(0)
    project(1, 0)
    in_res.wait()
    in_ups.wait()
    in_gain.wait()
    in_rg.wait()
    gain_row = gain_ref[...].reshape(1, WIDTH)
    cross_b(0)
    send_z(1, 3)
    send_z(1, 0)
    merge_a(0)
    merge_b(1)
    join_far(1)
    join_up(1)
    finish(0)
    join_down(1)
    cross_b(1)
    merge_a(1)
    gradient(0)
    finish(1)
    send_rest(0)
    forward_on("a", all_a, z, 0)
    forward_on("b", all_b, z, 0)
    gradient(1)
    send_rest(1)
    gain_c = message(gain0, gain0_rec, c_peer)

    order = [t, block_at(1 - z, 0), block_at(z, -1), block_at(z, 1), block_at(z, 2)]
    order += [block_at(1 - z, -1), block_at(1 - z, 1), block_at(1 - z, 2)]
    cx = {}

    def weight_grad(i):
        grad = jnp.concatenate([all_a[order[i]], all_b[order[i]]], axis=1)
        r = dot(grad, att[...], 0, 0).astype(BF16)
        for s in range(4):
            gwb[i, s % 2, s // 2] = r[s * OUT_ROWS : (s + 1) * OUT_ROWS]
        cx[i] = message(gwb.at[i, 1 - c], cx_rec.at[i], c_peer)

    low_rows, high_rows = pl.ds(0, HALF_ROWS), pl.ds(HALF_ROWS, HALF_ROWS)
    waits = []

    def has(i, d):
        return (x + d) % 4 // 2 == order[i] % 2

    z_waits = []

    def start_when(condition, *made, held=waits):
        held.extend((condition, make) for make in made)
        for make in made:
            make().start()

    def wait_when(condition, make):
        @pl.when(condition)
        def _():
            make().wait_send()

    X_SEM, Z_SEM = MESSAGES, MESSAGES + 48

    def x_copy(i, kind, src, step):
        sem = X_SEM + 6 * i + kind
        return pltpu.make_async_remote_copy(
            src_ref=src, dst_ref=x_rec.at[i, kind], send_sem=ssem.at[sem], recv_sem=rsem.at[sem],
            device_id=at_x(step), device_id_type=MESH,
        )

    def x_far(i, src, step):
        sem = X_SEM + 6 * i
        return pltpu.make_async_remote_copy(
            src_ref=src, dst_ref=x_rec.at[i, 0], send_sem=ssem.at[sem + (5 if step < 0 else 0)],
            recv_sem=rsem.at[sem], device_id=at_x(step), device_id_type=MESH,
        )

    def z_copy(kind, src, step):
        sem = Z_SEM + kind
        return pltpu.make_async_remote_copy(
            src_ref=src, dst_ref=z_rec.at[kind], send_sem=ssem.at[sem], recv_sem=rsem.at[sem],
            device_id=at_zh(step), device_id_type=MESH,
        )

    def x_first(i):
        cx[i].wait_recv()
        u[i] = gwb[i, c] + cx_rec[i]
        far, near, back_near = (x + 2) % 2, (x + 1) % 2, (x + 3) % 2
        is_far, is_next, is_back = has(i, 2), has(i, 1), has(i, 3)

        @pl.when(is_far)
        def _():
            start_when(
                is_far,
                lambda: x_far(i, u.at[i, far, low_rows], 1),
                lambda: x_far(i, u.at[i, far, high_rows], -1),
            )

        @pl.when(is_next)
        def _():
            start_when(is_next, lambda: x_copy(i, 1, u.at[i, near, high_rows], 1))

        @pl.when(is_back)
        def _():
            start_when(is_back, lambda: x_copy(i, 3, u.at[i, back_near, low_rows], -1))

    def x_second(i):
        near, back_near = (x + 1) % 2, (x + 3) % 2
        is_next, is_back = has(i, 1), has(i, 3)

        @pl.when(is_next)
        def _():
            x_far(i, x_mer.at[i], 1).wait_recv()
            x_mer[i] = u[i, near, :HALF_ROWS] + x_rec[i, 0]
            start_when(is_next, lambda: x_copy(i, 2, x_mer.at[i], 1))

        @pl.when(is_back)
        def _():
            x_far(i, x_mer.at[i], -1).wait_recv()
            x_mer[i] = u[i, back_near, HALF_ROWS:] + x_rec[i, 0]
            start_when(is_back, lambda: x_copy(i, 4, x_mer.at[i], -1))

    def x_last(i):
        kk = order[i] // 2
        e = (kk - zh) % 4
        mine = has(i, 0)
        is_far, is_next, is_back = mine & (e == 2), mine & (e == 1), mine & (e == 3)

        @pl.when(mine)
        def _():
            for kind in (1, 2, 3, 4):
                x_copy(i, kind, x_mer.at[i], 1).wait_recv()
            upper = u[i, x % 2, :HALF_ROWS].astype(F32) + x_rec[i, 2].astype(F32) + x_rec[i, 3].astype(F32)
            lower = u[i, x % 2, HALF_ROWS:].astype(F32) + x_rec[i, 1].astype(F32) + x_rec[i, 4].astype(F32)
            z_send[i, :HALF_ROWS] = upper.astype(BF16)
            z_send[i, HALF_ROWS:] = lower.astype(BF16)

            @pl.when(e == 0)
            def _():
                z_own[:HALF_ROWS] = upper
                z_own[HALF_ROWS:] = lower

        @pl.when(is_far)
        def _():
            start_when(
                is_far,
                lambda: z_copy(0, z_send.at[i, low_rows], 1),
                lambda: z_copy(1, z_send.at[i, high_rows], -1),
                held=z_waits,
            )

        @pl.when(is_next)
        def _():
            start_when(is_next, lambda: z_copy(2, z_send.at[i, high_rows], 1), held=z_waits)

        @pl.when(is_back)
        def _():
            start_when(is_back, lambda: z_copy(4, z_send.at[i, low_rows], -1), held=z_waits)

    def z_second(i):
        e = (order[i] // 2 - zh) % 4
        is_next, is_back = has(i, 0) & (e == 1), has(i, 0) & (e == 3)

        @pl.when(is_next)
        def _():
            z_copy(0, z_mer.at[0], 1).wait_recv()
            z_mer[0] = z_send[i, :HALF_ROWS] + z_rec[0]
            start_when(is_next, lambda: z_copy(3, z_mer.at[0], 1), held=z_waits)

        @pl.when(is_back)
        def _():
            z_copy(1, z_mer.at[1], -1).wait_recv()
            z_mer[1] = z_send[i, HALF_ROWS:] + z_rec[1]
            start_when(is_back, lambda: z_copy(5, z_mer.at[1], -1), held=z_waits)

    weight_grad(0)
    arrived("a", 0, 2)
    across(-1, 0)
    across(1, 0)
    partner(0)
    forward_on("a", all_a, z, 1)
    arrived("a", 0, 3)
    across(2, 0)
    forward_on("b", all_b, z, 1)
    partner(1)
    x_first(0)
    arrived("a", 1, 2)
    across(-1, 1)
    across(1, 1)
    arrived("b", 0, 2)
    arrived("b", 1, 2)
    weight_grad(2)
    weight_grad(3)
    forward_on("p", all_b, 1 - z, 0)
    x_first(2)
    x_first(3)
    ag["za", 0, 0].wait_recv()
    ag["za", 1, 0].wait_recv()
    weight_grad(1)
    gain_c.wait_recv()
    gain1[...] = gain0[...] + gain0_rec[...]
    gain_x = [message(gain1, gain1_rec.at[s - 1], at_x(s)) for s in (1, 2, 3)]
    x_second(0)
    accumulate(lambda j: t, True)
    x_first(1)
    arrived("a", 1, 3)
    across(2, 1)
    arrived("b", 0, 3)
    arrived("b", 1, 3)
    weight_grad(4)
    forward_on("p", all_b, 1 - z, 1)
    accumulate(lambda j: order[3] * j + order[2] * (1 - j), False)
    x_second(2)
    x_first(4)
    x_second(3)
    for n in (0, 1):
        ag["za", n, -1].wait_recv()
        ag["za", n, 1].wait_recv()
        arrived("p", n, 2)
    weight_grad(5)
    weight_grad(6)
    x_second(1)
    x_last(0)
    x_first(5)
    accumulate(lambda j: order[4] * j + order[1] * (1 - j), False)
    for n in (0, 1):
        ag["za", n, 2].wait_recv()
        arrived("p", n, 3)
    weight_grad(7)
    x_second(4)
    x_last(2)
    x_first(7)
    x_second(5)
    x_first(6)
    for copy in gain_x:
        copy.wait_recv()
    gain2[...] = gain1[...] + gain1_rec[0] + gain1_rec[1] + gain1_rec[2]
    gain_z = [message(gain2, gain2_rec.at[s - 1], at_zh(s)) for s in (1, 2, 3)]
    x_last(1)
    accumulate(lambda j: order[6] * j + order[5] * (1 - j), False)
    x_last(3)
    last = order[7]
    grad = jnp.concatenate([all_a[last], all_b[last]], axis=1)
    ga[...] = (gacc[...] + dot(grad, w[w_rows(last), :], 1, 0)).astype(BF16)
    x_last(4)
    x_second(6)
    z_second(0)
    x_second(7)

    def backward(h, carry):
        cols = head_cols(h)
        g_head = ga[:, cols]
        p = probs[h]
        gv[:, cols] = dot(p.astype(BF16), g_head, 0, 0).astype(BF16)
        gp = dot(g_head, v[:, cols], 1, 1)
        delta = jnp.sum(p * gp, axis=1, keepdims=True)
        gs = (p * (gp - delta) * SCALE).astype(BF16)
        gq[:, cols] = dot(gs, k[:, cols], 1, 0).astype(BF16)
        gk[:, cols] = dot(gs, q[:, cols], 0, 0).astype(BF16)
        return carry

    lax.fori_loop(0, 1, backward, 0)
    x_last(5)
    lax.fori_loop(1, 3, backward, 0)
    z_second(2)
    z_second(1)
    x_last(6)
    x_last(7)
    lax.fori_loop(3, HEADS, backward, 0)
    for copy in gain_z:
        copy.wait_recv()
    gain = gain2[...] + gain2_rec[0] + gain2_rec[1] + gain2_rec[2]
    gg_ref[...] = jnp.sum(gain, axis=0)
    for copy in messages:
        copy.wait_send()
    for condition, make in waits:
        wait_when(condition, make)
    z_second(3)
    z_second(4)
    z_second(5)
    z_second(6)
    z_second(7)

    for kind in (2, 3, 4, 5):
        z_copy(kind, z_mer.at[0], 1).wait_recv()
    gw_out[:HALF_ROWS] = z_own[:HALF_ROWS] + z_rec[3].astype(F32) + z_rec[4].astype(F32)
    gw_out[HALF_ROWS:] = z_own[HALF_ROWS:] + z_rec[2].astype(F32) + z_rec[5].astype(F32)

    for condition, make in z_waits:
        wait_when(condition, make)
    assert len(messages) <= MESSAGES


def hand_over(*refs):
    n = len(refs) // 2
    sources, outs, sems = refs[:n], refs[n : 2 * n], refs[2 * n]
    copies = [pltpu.make_async_copy(a, b, sems.at[i]) for i, (a, b) in enumerate(zip(sources, outs))]
    for copy in copies:
        copy.start()
    for copy in copies:
        copy.wait()


def deliver(arrays):
    vmem = pl.BlockSpec(memory_space=pltpu.VMEM)
    return pl.pallas_call(
        hand_over,
        out_shape=[jax.ShapeDtypeStruct(a.shape, a.dtype) for a in arrays],
        in_specs=[vmem] * len(arrays),
        out_specs=[pl.BlockSpec(memory_space=pl.ANY)] * len(arrays),
        scratch_shapes=[pltpu.SemaphoreType.DMA((len(arrays),))],
        compiler_params=pltpu.CompilerParams(vmem_limit_bytes=8 << 20),
    )(*arrays)


def shards(q, k, v, mask, res, w, gain, ups, rg):
    rows = jax.ShapeDtypeStruct((LEN, WIDTH), BF16)
    hbm = pl.BlockSpec(memory_space=pltpu.HBM)
    vmem = pl.BlockSpec(memory_space=pltpu.VMEM)

    def b(*shape):
        return pltpu.VMEM(shape, BF16)

    def f(*shape):
        return pltpu.VMEM(shape, F32)

    slab = (LEN, WIDTH)
    part = (OUT_ROWS, WIDTH)
    half = (HALF_ROWS, WIDTH)
    scratch = [
        b(*slab), b(*slab), b(*slab), pltpu.VMEM((1, LEN), jnp.int32), b(*slab), b(D, WIDTH), f(WIDTH), b(*slab), b(*slab),
        f(LEN, LEN), f(HEADS, LEN, LEN), b(*slab), b(*slab), f(*slab),
        b(4, 2, LEN, CA), b(4, 2, LEN, CB), b(4, LEN, CA), b(2, 6, QUARTER, CA), b(2, 6, 2, QUARTER, CB),
        b(2, 2, QUARTER, CA), b(2, 2, 2, QUARTER, CB), b(LEN, CB), b(LEN, CB), f(*slab),
        f(2, 8, 256), f(2, 8, 8, 256), b(8, LEN, CA), b(8, LEN, CB),
        b(8, 2, 2, *part), b(8, 2, *part), b(8, 2, *part), b(8, 5, *half), b(8, *half),
        b(8, *part), b(6, *half), b(2, *half), f(*part),
        f(8, WIDTH), f(8, WIDTH), f(8, WIDTH), f(3, 8, WIDTH), f(8, WIDTH), f(3, 8, WIDTH),
        pltpu.SemaphoreType.DMA((MESSAGES + 54,)),
        pltpu.SemaphoreType.DMA((MESSAGES + 54,)),
        pltpu.SemaphoreType.DMA((16,)),
    ]
    outs = pl.pallas_call(
        kernel,
        out_shape=(
            rows, rows, rows, rows, rows,
            jax.ShapeDtypeStruct(part, F32),
            jax.ShapeDtypeStruct((WIDTH,), F32),
        ),
        in_specs=[hbm] * 9,
        out_specs=(vmem,) * 7,
        scratch_shapes=scratch,
        compiler_params=pltpu.CompilerParams(
            collective_id=0, has_side_effects=True, vmem_limit_bytes=VMEM_LIMIT
        ),
    )(q, k, v, mask, res, w, gain, ups, rg)
    return deliver(outs)


def solution(mesh):
    placed = P("dp", "tensor")
    return jax.shard_map(
        shards,
        mesh=mesh,
        in_specs=(placed, placed, placed, P("dp", None), placed, P(None, "tensor"), P("tensor"), placed, placed),
        out_specs=(placed,) * 6 + (P("tensor"),),
        check_vma=False,
    )
```

```python
import functools

import jax
import jax.numpy as jnp
from jax import lax
from jax.experimental import pallas as pl
from jax.experimental.pallas import tpu as pltpu
from jax.sharding import PartitionSpec as P

MESH = pl.DeviceIdType.MESH
F32 = jnp.float32
BF16 = jnp.bfloat16

D = 5120
HEAD_DIM = 128
LEN = 384
WIDTH = 640
HEADS = WIDTH // HEAD_DIM
CA = 256
CB = WIDTH - CA
HALF = LEN // 2
QUARTER = HALF // 2
OUT_ROWS = 160
HALF_ROWS = OUT_ROWS // 2
SCALE = HEAD_DIM ** (-0.5)
EPSILON = 1e-05
MESSAGES = 128
VMEM_LIMIT = 51 << 20


def dot(a, b, ca, cb):
    return lax.dot_general(a, b, (((ca,), (cb,)), ((), ())), preferred_element_type=F32)


def kernel(
    q_hbm, k_hbm, v_hbm, mask_hbm, res_hbm, w_hbm, gain_hbm, ups_hbm, rg_hbm,
    lo, gr, gq, gk, gv, gw_out, gg_ref,
    q, k, v, mask_ref, res, w, gain_ref, ups, rg, bias, probs, att, ga, gacc,
    pa, pb, rec_az, rec_a, rec_b, mer_a, mer_b, zb_send, zb_rec, own,
    stat, stat_rec, all_a, all_b,
    gwb, cx_rec, u, x_rec, x_mer, z_send, z_rec, z_mer, z_own,
    gain0, gain0_rec, gain1, gain1_rec, gain2, gain2_rec,
    ssem, rsem, lsem,
):
    t = lax.axis_index("tensor")
    dp = lax.axis_index("dp")
    z, y = t // 4, t % 4
    c, x, zh = dp % 2, (dp // 2) % 4, dp // 8

    def at_y(step):
        return {"tensor": z * 4 + (y + step) % 4}

    z_peer = {"tensor": (1 - z) * 4 + y}
    c_peer = {"dp": dp + 1 - 2 * c}

    def at_x(step):
        return {"dp": zh * 8 + ((x + step) % 4) * 2 + c}

    def at_zh(step):
        return {"dp": ((zh + step) % 4) * 8 + x * 2 + c}

    peers = [{"tensor": (t + j) % 8} for j in range(1, 8)]
    peers += [c_peer]
    peers += [at_x(s) for s in (1, 2, 3)]
    peers += [at_zh(s) for s in (1, 2, 3)]

    local = []

    def fetch(src, dst):
        copy = pltpu.make_async_copy(src, dst, lsem.at[len(local)])
        local.append(copy)
        copy.start()
        return copy

    in_mask = fetch(mask_hbm, mask_ref)
    in_q, in_k, in_v = fetch(q_hbm, q), fetch(k_hbm, k), fetch(v_hbm, v)
    in_w = fetch(w_hbm, w)
    in_gain = fetch(gain_hbm, gain_ref)
    in_res, in_ups, in_rg = fetch(res_hbm, res), fetch(ups_hbm, ups), fetch(rg_hbm, rg)

    barrier = pltpu.get_barrier_semaphore()
    for peer in peers:
        pl.semaphore_signal(barrier, inc=1, device_id=peer, device_id_type=MESH)

    messages = []

    def message(src, dst, device, start=True):
        i = len(messages)
        copy = pltpu.make_async_remote_copy(
            src_ref=src, dst_ref=dst, send_sem=ssem.at[i], recv_sem=rsem.at[i],
            device_id=device, device_id_type=MESH,
        )
        messages.append(copy)
        if start:
            copy.start()
        return copy

    in_mask.wait()
    zeros = jnp.sum(1 - mask_ref[...], axis=1, keepdims=True)
    row = lax.broadcasted_iota(jnp.int32, (LEN, LEN), 0)
    col = lax.broadcasted_iota(jnp.int32, (LEN, LEN), 1)
    allowed = (col <= row) | (jnp.maximum(row, col) < zeros)
    bias[...] = jnp.where(allowed, 0.0, -jnp.inf).astype(F32)
    in_q.wait()
    in_k.wait()
    in_v.wait()

    def head_cols(h):
        return pl.ds(pl.multiple_of(h * HEAD_DIM, HEAD_DIM), HEAD_DIM)

    units = (pl.ds(0, HALF), pl.ds(HALF, HALF))
    firsts = (pl.ds(0, QUARTER), pl.ds(HALF, QUARTER))
    seconds = (pl.ds(QUARTER, QUARTER), pl.ds(HALF + QUARTER, QUARTER))

    def attend(n):
        rows = units[n]

        def forward(h, carry):
            cols = head_cols(h)
            s = dot(q[rows, cols], k[:, cols], 1, 1) * SCALE + bias[rows]
            e = jnp.exp(s - jnp.max(s, axis=1, keepdims=True))
            p = e * (1.0 / jnp.sum(e, axis=1, keepdims=True))
            probs[h, rows] = p
            att[rows, cols] = dot(p.astype(BF16), v[:, cols], 1, 0).astype(BF16)
            return carry

        lax.fori_loop(0, HEADS, forward, 0, unroll=True)

    def w_rows(block):
        return pl.ds(pl.multiple_of(block * WIDTH, WIDTH), WIDTH)

    def project(n, d):
        rows = units[n]

        def one(j, carry):
            zz = j * z + (1 - j) * (1 - z)
            block = zz * 4 + (y + d) % 4
            r = dot(att[rows], w[w_rows(block), :], 1, 1)
            pa[d, j, rows] = r[:, :CA].astype(BF16)
            pb[d, zz, rows] = r[:, CA:].astype(BF16)
            return carry

        lax.fori_loop(0, 2, one, 0)

    rs = {}

    def send_far(n):
        rs["b", n, 0] = message(pb.at[2, :, firsts[n]], rec_b.at[n, 0], at_y(1))
        rs["b", n, 1] = message(pb.at[2, :, seconds[n]], rec_b.at[n, 1], at_y(-1))

    def send_up(n):
        rs["b", n, 2] = message(pb.at[1, :, seconds[n]], rec_b.at[n, 2], at_y(1))

    def send_down(n):
        rs["b", n, 3] = message(pb.at[3, :, firsts[n]], rec_b.at[n, 3], at_y(-1))

    def send_z(n, d):
        rs["z", n, d] = message(pa.at[d, 0, units[n]], rec_az.at[d, units[n]], z_peer)

    def merge_b(n):
        rs["b", n, 0].wait_recv()
        mer_b[n, 0] = pb[1, :, firsts[n]] + rec_b[n, 0]
        rs["b", n, 4] = message(mer_b.at[n, 0], rec_b.at[n, 4], at_y(1))
        rs["b", n, 1].wait_recv()
        mer_b[n, 1] = pb[3, :, seconds[n]] + rec_b[n, 1]
        rs["b", n, 5] = message(mer_b.at[n, 1], rec_b.at[n, 5], at_y(-1))

    def join(n, d):
        rs["z", n, d].wait_recv()
        pa[d, 1, units[n]] = pa[d, 1, units[n]] + rec_az[d, units[n]]

    def join_far(n):
        join(n, 2)
        rs["a", n, 0] = message(pa.at[2, 1, firsts[n]], rec_a.at[n, 0], at_y(1))
        rs["a", n, 1] = message(pa.at[2, 1, seconds[n]], rec_a.at[n, 1], at_y(-1))

    def join_up(n):
        join(n, 1)
        rs["a", n, 2] = message(pa.at[1, 1, seconds[n]], rec_a.at[n, 2], at_y(1))

    def join_down(n):
        join(n, 3)
        rs["a", n, 3] = message(pa.at[3, 1, firsts[n]], rec_a.at[n, 3], at_y(-1))

    def merge_a(n):
        rs["a", n, 0].wait_recv()
        mer_a[n, 0] = pa[1, 1, firsts[n]] + rec_a[n, 0]
        rs["a", n, 4] = message(mer_a.at[n, 0], rec_a.at[n, 4], at_y(1))
        rs["a", n, 1].wait_recv()
        mer_a[n, 1] = pa[3, 1, seconds[n]] + rec_a[n, 1]
        rs["a", n, 5] = message(mer_a.at[n, 1], rec_a.at[n, 5], at_y(-1))

    def b_sum(n, zz):
        top = pb[0, zz, firsts[n]].astype(F32) + rec_b[n, 3, zz].astype(F32) + rec_b[n, 4, zz].astype(F32)
        low = pb[0, zz, seconds[n]].astype(F32) + rec_b[n, 2, zz].astype(F32) + rec_b[n, 5, zz].astype(F32)
        return top, low

    def cross_b(n):
        for i in (2, 3, 4, 5):
            rs["b", n, i].wait_recv()
        top, low = b_sum(n, 1 - z)
        zb_send[firsts[n]] = top.astype(BF16)
        zb_send[seconds[n]] = low.astype(BF16)
        rs["zb", n] = message(zb_send.at[units[n]], zb_rec.at[units[n]], z_peer)
        top, low = b_sum(n, z)
        own[firsts[n], CA:] = top
        own[seconds[n], CA:] = low

    def finish(n):
        rows = units[n]
        rs["z", n, 0].wait_recv()
        for i in (2, 3, 4, 5):
            rs["a", n, i].wait_recv()
        add_top = rec_a[n, 3].astype(F32) + rec_a[n, 4].astype(F32)
        add_low = rec_a[n, 2].astype(F32) + rec_a[n, 5].astype(F32)
        for part, add in ((firsts[n], add_top), (seconds[n], add_low)):
            total = pa[0, 1, part].astype(F32) + rec_az[0, part].astype(F32) + add
            lo[part, :CA] = (total + res[part, :CA].astype(F32)).astype(BF16)
        f_a = lo[rows, :CA].astype(F32)
        scaled_a = ups[rows, :CA].astype(F32) * gain_row[:, :CA]
        square = jnp.sum(f_a * f_a, axis=1, keepdims=True)
        inner = jnp.sum(f_a * scaled_a, axis=1, keepdims=True)
        rs["zb", n].wait_recv()
        own_b = own[rows, CA:] + zb_rec[rows].astype(F32) + res[rows, CA:].astype(F32)
        low_b = own_b.astype(BF16)
        lo[rows, CA:] = low_b
        f_b = low_b.astype(F32)
        scaled_b = ups[rows, CA:].astype(F32) * gain_row[:, CA:]
        square = square + jnp.sum(f_b * f_b, axis=1, keepdims=True)
        inner = inner + jnp.sum(f_b * scaled_b, axis=1, keepdims=True)
        lane = lax.broadcasted_iota(jnp.int32, (HALF, 128), 1)
        packed = jnp.where(lane == 0, square, jnp.where(lane == 1, inner, 0.0))
        packed = jnp.concatenate([packed, jnp.zeros((64, 128), F32)], axis=0)
        stat[n] = packed.T[:8]
        for j in range(1, 8):
            rs["s", n, j] = message(stat.at[n], stat_rec.at[n, j], peers[j - 1])

    ag = {}

    def gradient(n):
        rows = units[n]
        total = stat[n]
        for j in range(1, 8):
            rs["s", n, j].wait_recv()
            total = total + stat_rec[n, j]
        wide = jnp.concatenate([total, jnp.zeros((120, 256), F32)], axis=0).T[:HALF]
        square, inner = wide[:, 0:1], wide[:, 1:2]
        rms = jnp.sqrt(square / D + EPSILON)
        back = 1.0 / rms
        row_inner = inner / (rms * D)
        cut = (slice(0, CA), slice(CA, WIDTH))
        for buf, cols in zip((all_a, all_b), cut):
            up = ups[rows, cols].astype(F32)
            normed = lo[rows, cols].astype(F32) * back
            g = rg[rows, cols].astype(F32) + (up * gain_row[:, cols] - normed * row_inner) * back
            g = g.astype(BF16)
            buf[t, rows] = g
            gr[rows, cols] = g
            share = (up * normed).reshape(HALF // 8, 8, -1).sum(axis=0)
            if n == 0:
                gain0[:, cols] = share
            else:
                gain0[:, cols] += share
        ag["zb", n] = message(all_b.at[t, rows], all_b.at[t, rows], z_peer)
        for key, buf in (("a", all_a), ("b", all_b)):
            send_half(key, buf, t, n, 1, firsts[n], 1)
            send_half(key, buf, t, n, -1, seconds[n], 1)

    def send_rest(n):
        rows = units[n]
        ag["za", n, 0] = message(all_a.at[t, rows], all_a.at[t, rows], z_peer)
        for key, buf in (("a", all_a), ("b", all_b)):
            send_half(key, buf, t, n, 1, seconds[n], 2)
            send_half(key, buf, t, n, -1, firsts[n], 2)

    def send_half(key, buf, block, n, step, rows, turn):
        part = buf.at[block, rows]
        ag[key, n, step, turn] = message(part, part, at_y(step))

    def block_at(zz, step):
        return zz * 4 + (y + step) % 4

    def forward_on(key, buf, zz, n):
        ag[key, n, 1, 1].wait_recv()
        send_half(key, buf, block_at(zz, -1), n, 1, firsts[n], 3)
        ag[key, n, -1, 1].wait_recv()
        send_half(key, buf, block_at(zz, 1), n, -1, seconds[n], 3)

    def arrived(key, n, turn):
        ag[key, n, 1, turn].wait_recv()
        ag[key, n, -1, turn].wait_recv()

    def partner(n):
        ag["zb", n].wait_recv()
        block = block_at(1 - z, 0)
        send_half("p", all_b, block, n, 1, firsts[n], 1)
        send_half("p", all_b, block, n, -1, seconds[n], 1)
        send_half("p", all_b, block, n, 1, seconds[n], 2)
        send_half("p", all_b, block, n, -1, firsts[n], 2)

    def across(step, n):
        part = all_a.at[block_at(z, step), units[n]]
        ag["za", n, step] = message(part, part, z_peer)

    def accumulate(blocks, start):
        def one(j, carry):
            block = blocks(j)
            grad = jnp.concatenate([all_a[block], all_b[block]], axis=1)
            r = dot(grad, w[w_rows(block), :], 1, 0)
            if start:
                gacc[...] = r
            else:
                gacc[...] += r
            return carry

        lax.fori_loop(0, 1 if start else 2, one, 0)

    attend(0)
    in_w.wait()
    project(0, 2)
    pl.semaphore_wait(barrier, len(peers))
    send_far(0)
    send_z(0, 2)
    project(0, 1)
    send_up(0)
    send_z(0, 1)
    project(0, 3)
    send_down(0)
    send_z(0, 3)
    project(0, 0)
    send_z(0, 0)
    attend(1)
    project(1, 2)
    merge_b(0)
    send_far(1)
    send_z(1, 2)
    join_far(0)
    project(1, 1)
    send_up(1)
    send_z(1, 1)
    project(1, 3)
    send_down(1)
    join_up(0)
    join_down(0)
    project(1, 0)
    in_res.wait()
    in_ups.wait()
    in_gain.wait()
    in_rg.wait()
    gain_row = gain_ref[...].reshape(1, WIDTH)
    cross_b(0)
    send_z(1, 3)
    send_z(1, 0)
    merge_a(0)
    merge_b(1)
    join_far(1)
    join_up(1)
    finish(0)
    join_down(1)
    cross_b(1)
    merge_a(1)
    gradient(0)
    finish(1)
    send_rest(0)
    forward_on("a", all_a, z, 0)
    forward_on("b", all_b, z, 0)
    gradient(1)
    send_rest(1)
    gain_c = message(gain0, gain0_rec, c_peer)

    order = [t, block_at(1 - z, 0), block_at(z, -1), block_at(z, 1), block_at(z, 2)]
    order += [block_at(1 - z, -1), block_at(1 - z, 1), block_at(1 - z, 2)]
    cx = {}

    def weight_grad(i):
        grad = jnp.concatenate([all_a[order[i]], all_b[order[i]]], axis=1)
        r = dot(grad, att[...], 0, 0).astype(BF16)
        for s in range(4):
            gwb[i, s % 2, s // 2] = r[s * OUT_ROWS : (s + 1) * OUT_ROWS]
        cx[i] = message(gwb.at[i, 1 - c], cx_rec.at[i], c_peer)

    low_rows, high_rows = pl.ds(0, HALF_ROWS), pl.ds(HALF_ROWS, HALF_ROWS)
    waits = []

    def has(i, d):
        return (x + d) % 4 // 2 == order[i] % 2

    z_waits = []

    def start_when(condition, *made, held=waits):
        held.extend((condition, make) for make in made)
        for make in made:
            make().start()

    def wait_when(condition, make):
        @pl.when(condition)
        def _():
            make().wait_send()

    X_SEM, Z_SEM = MESSAGES, MESSAGES + 48

    def x_copy(i, kind, src, step):
        sem = X_SEM + 6 * i + kind
        return pltpu.make_async_remote_copy(
            src_ref=src, dst_ref=x_rec.at[i, kind], send_sem=ssem.at[sem], recv_sem=rsem.at[sem],
            device_id=at_x(step), device_id_type=MESH,
        )

    def x_far(i, src, step):
        sem = X_SEM + 6 * i
        return pltpu.make_async_remote_copy(
            src_ref=src, dst_ref=x_rec.at[i, 0], send_sem=ssem.at[sem + (5 if step < 0 else 0)],
            recv_sem=rsem.at[sem], device_id=at_x(step), device_id_type=MESH,
        )

    def z_copy(kind, src, step):
        sem = Z_SEM + kind
        return pltpu.make_async_remote_copy(
            src_ref=src, dst_ref=z_rec.at[kind], send_sem=ssem.at[sem], recv_sem=rsem.at[sem],
            device_id=at_zh(step), device_id_type=MESH,
        )

    def x_first(i):
        cx[i].wait_recv()
        u[i] = gwb[i, c] + cx_rec[i]
        far, near, back_near = (x + 2) % 2, (x + 1) % 2, (x + 3) % 2
        is_far, is_next, is_back = has(i, 2), has(i, 1), has(i, 3)

        @pl.when(is_far)
        def _():
            start_when(
                is_far,
                lambda: x_far(i, u.at[i, far, low_rows], 1),
                lambda: x_far(i, u.at[i, far, high_rows], -1),
            )

        @pl.when(is_next)
        def _():
            start_when(is_next, lambda: x_copy(i, 1, u.at[i, near, high_rows], 1))

        @pl.when(is_back)
        def _():
            start_when(is_back, lambda: x_copy(i, 3, u.at[i, back_near, low_rows], -1))

    def x_second(i):
        near, back_near = (x + 1) % 2, (x + 3) % 2
        is_next, is_back = has(i, 1), has(i, 3)

        @pl.when(is_next)
        def _():
            x_far(i, x_mer.at[i], 1).wait_recv()
            x_mer[i] = u[i, near, :HALF_ROWS] + x_rec[i, 0]
            start_when(is_next, lambda: x_copy(i, 2, x_mer.at[i], 1))

        @pl.when(is_back)
        def _():
            x_far(i, x_mer.at[i], -1).wait_recv()
            x_mer[i] = u[i, back_near, HALF_ROWS:] + x_rec[i, 0]
            start_when(is_back, lambda: x_copy(i, 4, x_mer.at[i], -1))

    def x_last(i):
        kk = order[i] // 2
        e = (kk - zh) % 4
        mine = has(i, 0)
        is_far, is_next, is_back = mine & (e == 2), mine & (e == 1), mine & (e == 3)

        @pl.when(mine)
        def _():
            for kind in (1, 2, 3, 4):
                x_copy(i, kind, x_mer.at[i], 1).wait_recv()
            upper = u[i, x % 2, :HALF_ROWS].astype(F32) + x_rec[i, 2].astype(F32) + x_rec[i, 3].astype(F32)
            lower = u[i, x % 2, HALF_ROWS:].astype(F32) + x_rec[i, 1].astype(F32) + x_rec[i, 4].astype(F32)
            z_send[i, :HALF_ROWS] = upper.astype(BF16)
            z_send[i, HALF_ROWS:] = lower.astype(BF16)

            @pl.when(e == 0)
            def _():
                z_own[:HALF_ROWS] = upper
                z_own[HALF_ROWS:] = lower

        @pl.when(is_far)
        def _():
            start_when(
                is_far,
                lambda: z_copy(0, z_send.at[i, low_rows], 1),
                lambda: z_copy(1, z_send.at[i, high_rows], -1),
                held=z_waits,
            )

        @pl.when(is_next)
        def _():
            start_when(is_next, lambda: z_copy(2, z_send.at[i, high_rows], 1), held=z_waits)

        @pl.when(is_back)
        def _():
            start_when(is_back, lambda: z_copy(4, z_send.at[i, low_rows], -1), held=z_waits)

    def z_second(i):
        e = (order[i] // 2 - zh) % 4
        is_next, is_back = has(i, 0) & (e == 1), has(i, 0) & (e == 3)

        @pl.when(is_next)
        def _():
            z_copy(0, z_mer.at[0], 1).wait_recv()
            z_mer[0] = z_send[i, :HALF_ROWS] + z_rec[0]
            start_when(is_next, lambda: z_copy(3, z_mer.at[0], 1), held=z_waits)

        @pl.when(is_back)
        def _():
            z_copy(1, z_mer.at[1], -1).wait_recv()
            z_mer[1] = z_send[i, HALF_ROWS:] + z_rec[1]
            start_when(is_back, lambda: z_copy(5, z_mer.at[1], -1), held=z_waits)

    weight_grad(0)
    arrived("a", 0, 2)
    across(-1, 0)
    across(1, 0)
    partner(0)
    forward_on("a", all_a, z, 1)
    arrived("a", 0, 3)
    across(2, 0)
    forward_on("b", all_b, z, 1)
    partner(1)
    x_first(0)
    arrived("a", 1, 2)
    across(-1, 1)
    across(1, 1)
    arrived("b", 0, 2)
    arrived("b", 1, 2)
    weight_grad(2)
    weight_grad(3)
    forward_on("p", all_b, 1 - z, 0)
    x_first(2)
    x_first(3)
    ag["za", 0, 0].wait_recv()
    ag["za", 1, 0].wait_recv()
    weight_grad(1)
    gain_c.wait_recv()
    gain1[...] = gain0[...] + gain0_rec[...]
    gain_x = [message(gain1, gain1_rec.at[s - 1], at_x(s)) for s in (1, 2, 3)]
    x_second(0)
    accumulate(lambda j: t, True)
    x_first(1)
    arrived("a", 1, 3)
    across(2, 1)
    arrived("b", 0, 3)
    arrived("b", 1, 3)
    weight_grad(4)
    forward_on("p", all_b, 1 - z, 1)
    accumulate(lambda j: order[3] * j + order[2] * (1 - j), False)
    x_second(2)
    x_first(4)
    x_second(3)
    for n in (0, 1):
        ag["za", n, -1].wait_recv()
        ag["za", n, 1].wait_recv()
        arrived("p", n, 2)
    weight_grad(5)
    weight_grad(6)
    x_second(1)
    x_last(0)
    x_first(5)
    accumulate(lambda j: order[4] * j + order[1] * (1 - j), False)
    for n in (0, 1):
        ag["za", n, 2].wait_recv()
        arrived("p", n, 3)
    weight_grad(7)
    x_second(4)
    x_last(2)
    x_first(7)
    x_second(5)
    x_first(6)
    for copy in gain_x:
        copy.wait_recv()
    gain2[...] = gain1[...] + gain1_rec[0] + gain1_rec[1] + gain1_rec[2]
    gain_z = [message(gain2, gain2_rec.at[s - 1], at_zh(s)) for s in (1, 2, 3)]
    x_last(1)
    accumulate(lambda j: order[6] * j + order[5] * (1 - j), False)
    x_last(3)
    last = order[7]
    grad = jnp.concatenate([all_a[last], all_b[last]], axis=1)
    ga[...] = (gacc[...] + dot(grad, w[w_rows(last), :], 1, 0)).astype(BF16)
    x_last(4)
    x_second(6)
    z_second(0)
    x_second(7)

    def backward(h, carry):
        cols = head_cols(h)
        g_head = ga[:, cols]
        p = probs[h]
        gv[:, cols] = dot(p.astype(BF16), g_head, 0, 0).astype(BF16)
        gp = dot(g_head, v[:, cols], 1, 1)
        delta = jnp.sum(p * gp, axis=1, keepdims=True)
        gs = (p * (gp - delta) * SCALE).astype(BF16)
        gq[:, cols] = dot(gs, k[:, cols], 1, 0).astype(BF16)
        gk[:, cols] = dot(gs, q[:, cols], 0, 0).astype(BF16)
        return carry

    lax.fori_loop(0, 1, backward, 0)
    x_last(5)
    lax.fori_loop(1, 3, backward, 0)
    z_second(2)
    z_second(1)
    x_last(7)
    x_last(6)
    z_second(3)
    z_second(4)
    z_second(5)
    lax.fori_loop(3, HEADS, backward, 0)
    for copy in gain_z:
        copy.wait_recv()
    gain = gain2[...] + gain2_rec[0] + gain2_rec[1] + gain2_rec[2]
    gg_ref[...] = jnp.sum(gain, axis=0)
    for copy in messages:
        copy.wait_send()
    for condition, make in waits:
        wait_when(condition, make)
    z_second(7)
    z_second(6)

    for kind in (2, 3, 4, 5):
        z_copy(kind, z_mer.at[0], 1).wait_recv()
    gw_out[:HALF_ROWS] = z_own[:HALF_ROWS] + z_rec[3].astype(F32) + z_rec[4].astype(F32)
    gw_out[HALF_ROWS:] = z_own[HALF_ROWS:] + z_rec[2].astype(F32) + z_rec[5].astype(F32)

    for condition, make in z_waits:
        wait_when(condition, make)
    assert len(messages) <= MESSAGES


def hand_over(*refs):
    n = len(refs) // 2
    sources, outs, sems = refs[:n], refs[n : 2 * n], refs[2 * n]
    copies = [pltpu.make_async_copy(a, b, sems.at[i]) for i, (a, b) in enumerate(zip(sources, outs))]
    for copy in copies:
        copy.start()
    for copy in copies:
        copy.wait()


def deliver(arrays):
    vmem = pl.BlockSpec(memory_space=pltpu.VMEM)
    return pl.pallas_call(
        hand_over,
        out_shape=[jax.ShapeDtypeStruct(a.shape, a.dtype) for a in arrays],
        in_specs=[vmem] * len(arrays),
        out_specs=[pl.BlockSpec(memory_space=pl.ANY)] * len(arrays),
        scratch_shapes=[pltpu.SemaphoreType.DMA((len(arrays),))],
        compiler_params=pltpu.CompilerParams(vmem_limit_bytes=8 << 20),
    )(*arrays)


def shards(q, k, v, mask, res, w, gain, ups, rg):
    rows = jax.ShapeDtypeStruct((LEN, WIDTH), BF16)
    hbm = pl.BlockSpec(memory_space=pltpu.HBM)
    vmem = pl.BlockSpec(memory_space=pltpu.VMEM)

    def b(*shape):
        return pltpu.VMEM(shape, BF16)

    def f(*shape):
        return pltpu.VMEM(shape, F32)

    slab = (LEN, WIDTH)
    part = (OUT_ROWS, WIDTH)
    half = (HALF_ROWS, WIDTH)
    scratch = [
        b(*slab), b(*slab), b(*slab), pltpu.VMEM((1, LEN), jnp.int32), b(*slab), b(D, WIDTH), f(WIDTH), b(*slab), b(*slab),
        f(LEN, LEN), f(HEADS, LEN, LEN), b(*slab), b(*slab), f(*slab),
        b(4, 2, LEN, CA), b(4, 2, LEN, CB), b(4, LEN, CA), b(2, 6, QUARTER, CA), b(2, 6, 2, QUARTER, CB),
        b(2, 2, QUARTER, CA), b(2, 2, 2, QUARTER, CB), b(LEN, CB), b(LEN, CB), f(*slab),
        f(2, 8, 256), f(2, 8, 8, 256), b(8, LEN, CA), b(8, LEN, CB),
        b(8, 2, 2, *part), b(8, 2, *part), b(8, 2, *part), b(8, 5, *half), b(8, *half),
        b(8, *part), b(6, *half), b(2, *half), f(*part),
        f(8, WIDTH), f(8, WIDTH), f(8, WIDTH), f(3, 8, WIDTH), f(8, WIDTH), f(3, 8, WIDTH),
        pltpu.SemaphoreType.DMA((MESSAGES + 54,)),
        pltpu.SemaphoreType.DMA((MESSAGES + 54,)),
        pltpu.SemaphoreType.DMA((16,)),
    ]
    outs = pl.pallas_call(
        kernel,
        out_shape=(
            rows, rows, rows, rows, rows,
            jax.ShapeDtypeStruct(part, F32),
            jax.ShapeDtypeStruct((WIDTH,), F32),
        ),
        in_specs=[hbm] * 9,
        out_specs=(vmem,) * 7,
        scratch_shapes=scratch,
        compiler_params=pltpu.CompilerParams(
            collective_id=0, has_side_effects=True, vmem_limit_bytes=VMEM_LIMIT
        ),
    )(q, k, v, mask, res, w, gain, ups, rg)
    return deliver(outs)


def solution(mesh):
    placed = P("dp", "tensor")
    return jax.shard_map(
        shards,
        mesh=mesh,
        in_specs=(placed, placed, placed, P("dp", None), placed, P(None, "tensor"), P("tensor"), placed, placed),
        out_specs=(placed,) * 6 + (P("tensor"),),
        check_vma=False,
    )
```
